32 devices in a mesh: ep: 4 (over y, x), edp: 4 (over z), tp: 2 (over core).
Axes of the slice: x: 2, y: 2, z: 4, core: 2. Of those that a mesh axis runs over, the one named last changes fastest.
Arguments:
- tokens: bfloat16 [2048, 4096], P(('ep', 'edp'), 'tp'), may hold values from -6 to 6
- cotangent: bfloat16 [2048, 4096], P(('ep', 'edp'), 'tp'), may hold values from -6 to 6
- expert_ids: int32 [2048, 8], P(('ep', 'edp')), may hold values from 0 to 127, all different within a row; in each aligned block of 128 rows (0 to 127, 128 to 255, ...) at most 10 rows name the same one
- route_weights: float32 [2048, 8], P(('ep', 'edp')), may hold values from 0.1 to 1
- expert_weights: bfloat16 [3, 1536, 4096], P(None, ('ep', 'tp')), may hold values from -0.15625 to 0.15625
Outputs:
- mixed: bfloat16 [2048, 4096], P(('ep', 'edp'), 'tp')
- grad_tokens: bfloat16 [2048, 4096], P(('ep', 'edp'), 'tp')
- weight_grads: float32 [3, 1536, 4096], P(None, ('ep', 'tp'), 'edp')
The draws below stay inside these ranges and needn't reach their ends.
Inputs may be any that keep to these rules, and one draw needn't show every extreme that they name: `expert_ids`: each token names 8 different experts; within the tokens of one (ep, edp) index no expert is named by more than 10 tokens.
All inputs are finite; a program needn't handle non-finite values.
Results may differ from the reference program's by a relative error of at most 0.017.
Values may be sent and summed in bfloat16 or wider, within the bound.
A program may use at most 64 MiB of HBM per device.

```python
import math
import jax
import jax.numpy as jnp
import numpy as np
from jax import lax

D = 4096
FF = 1536
EXPERTS = 128
TOP = 8
TOK_DEV = 128
CAP = 10
EXP_WIN = 1
SLICE = 192
TOKENS = 2048
N_EP = 4
N_EDP = 4
N_TP = 2


def block_levels(key, extent, shards, least, high):
    factor_of = 1.0
    for axis_at, blocks in shards:
        heights = jax.random.uniform(jax.random.fold_in(jax.random.fold_in(key, 6), axis_at), (blocks,), jnp.float32, least / len(shards), high / len(shards))
        factor_of = factor_of * jnp.repeat(jnp.exp(heights), extent[axis_at] // blocks).reshape((-1,) + (1,) * (len(extent) - 1 - axis_at))
    return factor_of


def deal_out(rng, own, number, rows, count, top, limit, slope):
    sequence = jax.random.permutation(rng, count)
    heavy_load, common = load_shares(count, rows * top, limit, slope, True), load_shares(count, rows * top, limit, slope, False)
    places = jnp.arange(count)

    def named(sizes, turn):
        used = int((sizes > 0).sum())
        fixed = max(1, used // 4)
        passed = fixed + (places - fixed + turn * (used - fixed)) % max(1, count - fixed)
        return jnp.zeros((count,), jnp.int32).at[sequence[jnp.where(places < fixed, places, passed)]].set(jnp.asarray(sizes, jnp.int32))

    sizes = jnp.where(number % 4 == 0, named(heavy_load, number // 4), named(common, number - number // 4 - 1))
    mixed = jax.random.permutation(jax.random.fold_in(own, 3), count)
    donor, taker = mixed[0:count // 2 * 2:2], mixed[1:count // 2 * 2:2]
    margin = jnp.minimum(sizes[donor] - 1, limit - sizes[taker]) // 2
    margin = jnp.where((donor == sequence[0]) | (taker == sequence[0]) | (sizes[taker] == 0), 0, jnp.maximum(margin, 0))
    passed = jax.random.randint(jax.random.fold_in(own, 4), (count // 2,), 0, 1 << 20) % (margin + 1)
    sizes = sizes.at[donor].add(-passed).at[taker].add(passed)
    labels = jnp.searchsorted(jnp.cumsum(sizes), jnp.arange(rows * top), side="right").astype(jnp.int32)
    listing = labels.reshape(top, rows).T
    listing = listing[jax.random.permutation(jax.random.fold_in(own, 1), rows)]
    turn = jax.random.randint(jax.random.fold_in(own, 2), (rows, 1), 0, top)
    return jnp.take_along_axis(listing, (jnp.arange(top)[None, :] + turn) % top, axis=1)


def load_shares(count, total, bound, lean, full):
    loads = [(1 << 20) // math.isqrt(standing ** lean) + 1 for standing in range(1, count + 1)]
    largest = bound if full else min(bound, max(-(-total // count), total * loads[0] // sum(loads)))
    least = 1 if total - largest >= count - 1 else 0
    counts, surplus = [largest] + [least] * (count - 1), total - largest - least * (count - 1)
    while surplus > 0:
        movable = [i for i in range(1, count) if counts[i] < largest] or [i for i in range(1, count) if counts[i] < bound]
        pool, remaining = sum([loads[i] for i in movable]), surplus
        for i in movable:
            addition = min(bound - counts[i], max(1, remaining * loads[i] // pool), surplus)
            counts[i] = counts[i] + addition
            surplus = surplus - addition
    return np.array(counts)


def noise(rng, shape, width, most, cuts=(), held_as=jnp.bfloat16):
    loudness = block_levels(rng, shape, cuts, -0.22, 0.18) if cuts else 1.0
    result = jax.random.normal(rng, shape, jnp.float32) * width * loudness
    return jnp.minimum(jnp.maximum(result, -most), most).astype(held_as)


def setup_inputs(seed: int = 0) -> dict:
    splits = jax.random.split(jax.random.key(seed), 6)
    tokens = noise(splits[0], (TOKENS, D), 1.0, 6.0, ((0, 16), (1, 2)))
    cotangent = noise(splits[1], (TOKENS, D), 1.0, 6.0, ((0, 16), (1, 2)))
    expert_ids_keys = jax.random.split(jax.random.fold_in(splits[2], 1), TOKENS // TOK_DEV)
    expert_ids_turns = jax.random.permutation(jax.random.fold_in(splits[2], 3), TOKENS // TOK_DEV)
    expert_ids = jax.vmap(lambda own, number: deal_out(jax.random.fold_in(splits[2], 2), own, number, TOK_DEV, EXPERTS, TOP, CAP, 1))(expert_ids_keys, expert_ids_turns).reshape((TOKENS, TOP))
    route_weights = jnp.clip(jnp.exp(math.log(1.0) - 2.3025851 * jax.random.uniform(splits[3], (TOKENS, TOP), jnp.float32) ** block_levels(splits[3], (TOKENS, TOP), ((0, 16),), -0.2, 0.2)), 0.1, 1.0)
    expert_weights = noise(splits[4], (3, EXP_WIN * FF, D), FF ** -0.5, 0.15625, ((1, 8),))
    return {"tokens": tokens, "cotangent": cotangent, "expert_ids": expert_ids, "route_weights": route_weights, "expert_weights": expert_weights}


def settle(values):
    return lax.optimization_barrier(values.astype(jnp.bfloat16)).astype(jnp.float32)


def reference(tokens, cotangent, expert_ids, route_weights, expert_weights):
    groups = N_EP * N_EDP
    window = N_EP // 4
    per_group = TOK_DEV * TOP
    flat_ids = expert_ids.reshape(groups, per_group)
    matches = (flat_ids[:, :, None] == jnp.arange(window, dtype=jnp.int32)[None, None, :]).astype(jnp.int32)
    slot_index = jnp.sum(matches * (jnp.cumsum(matches, axis=1) - 1), axis=2).astype(jnp.int32)
    owner = jnp.where(jnp.sum(matches, axis=2) > 0, flat_ids, window).astype(jnp.int32)
    token_index = (jnp.arange(groups, dtype=jnp.int32)[:, None] * TOK_DEV
                   + jnp.arange(per_group, dtype=jnp.int32)[None, :] // TOP).astype(jnp.int32)
    group_index = jnp.broadcast_to(jnp.arange(groups, dtype=jnp.int32)[:, None], flat_ids.shape).astype(jnp.int32)
    slot_token = jnp.zeros((window, groups, CAP), jnp.int32).at[owner, group_index, slot_index].set(token_index, mode="drop")
    slot_weight = jnp.zeros((window, groups, CAP), jnp.float32).at[owner, group_index, slot_index].set(
        route_weights.reshape(groups, per_group), mode="drop")
    slot_live = jnp.zeros((window, groups, CAP), jnp.float32).at[owner, group_index, slot_index].set(
        jnp.ones((groups, per_group), jnp.float32), mode="drop")
    expert_blocks = jnp.moveaxis(expert_weights.reshape(3, window, 4, N_TP, SLICE, D), 1, 0)
    row_count = groups * CAP

    def one_expert(operands):
        slot_toks, slot_wts, slot_flags, blocks = operands
        flat_tok = slot_toks.reshape(-1)
        live_col = slot_flags.reshape(-1, 1)
        rows = tokens[flat_tok] * live_col.astype(jnp.bfloat16)
        scaled = (cotangent[flat_tok].astype(jnp.float32) * (slot_wts.reshape(-1, 1) * live_col)).astype(jnp.bfloat16)
        rows_wide = rows.astype(jnp.float32).reshape(N_EP, N_EDP, CAP, D)
        scaled_wide = scaled.astype(jnp.float32).reshape(N_EP, N_EDP, CAP, D)

        def per_replica(left, right_wide):
            left_wide = left.astype(jnp.float32).reshape(N_EP, N_EDP, CAP, SLICE)
            partial_sums = jnp.einsum("pics,picd->isd", left_wide, right_wide, precision=lax.Precision.HIGHEST)
            return jnp.sum(settle(partial_sums), axis=0)

        def one_slice(carry, slab):
            out_acc, back_acc = carry
            gate_w, up_w, down_w = slab[0], slab[1], slab[2]
            gate_val = jnp.dot(rows, gate_w.T, preferred_element_type=jnp.float32)
            up_val = jnp.dot(rows, up_w.T, preferred_element_type=jnp.float32)
            sigmoid_gate = jax.nn.sigmoid(gate_val)
            active = gate_val * sigmoid_gate
            hidden = (active * up_val).astype(jnp.bfloat16)
            out_part = jnp.dot(hidden, down_w, preferred_element_type=jnp.float32)
            d_hidden = jnp.dot(scaled, down_w.T, preferred_element_type=jnp.float32)
            d_gate = (d_hidden * up_val * sigmoid_gate * (1.0 + gate_val * (1.0 - sigmoid_gate))).astype(jnp.bfloat16)
            d_up = (d_hidden * active).astype(jnp.bfloat16)
            back_part = (jnp.dot(d_gate, gate_w, preferred_element_type=jnp.float32)
                         + jnp.dot(d_up, up_w, preferred_element_type=jnp.float32))
            grad_slab = jnp.stack([per_replica(d_gate, rows_wide), per_replica(d_up, rows_wide),
                                   per_replica(hidden, scaled_wide)])
            return (out_acc + settle(out_part), back_acc + settle(back_part)), grad_slab

        out_total = jnp.zeros((row_count, D), jnp.float32)
        back_total = jnp.zeros((row_count, D), jnp.float32)
        grad_list = []
        for half_index in range(4):
            start = (jnp.zeros((row_count, D), jnp.float32), jnp.zeros((row_count, D), jnp.float32))
            slabs = jnp.moveaxis(blocks[:, half_index], 1, 0)
            (out_half, back_half), grad_half = lax.scan(one_slice, start, slabs)
            out_total = out_total + settle(out_half)
            back_total = back_total + settle(back_half)
            grad_list.append(grad_half)
        return out_total, back_total, jnp.stack(grad_list)

    outs, backs, grads = lax.map(one_expert, (slot_token, slot_weight, slot_live, expert_blocks))
    weight_grads = jnp.moveaxis(grads, 3, 0).reshape(3, window * FF, D)
    flat_tok = slot_token.reshape(-1)
    mixed = jnp.zeros((groups * TOK_DEV, D), jnp.float32).at[flat_tok].add(
        (slot_weight * slot_live).reshape(-1, 1) * outs.reshape(-1, D)).astype(jnp.bfloat16)
    grad_tokens = jnp.zeros((groups * TOK_DEV, D), jnp.float32).at[flat_tok].add(
        slot_live.reshape(-1, 1) * backs.reshape(-1, D)).astype(jnp.bfloat16)
    return mixed, grad_tokens, weight_grads
```

```python
import functools
import math

import jax
import jax.numpy as jnp
import numpy as np
from jax import lax
from jax.experimental import pallas as pl
from jax.experimental.pallas import tpu as pltpu
from jax.sharding import PartitionSpec as P

CAP = 10
PARTS = 4
SUB = 2
VMEM_LIMIT = 40 * 1024 * 1024
MESH = pl.DeviceIdType.MESH
F32 = jnp.float32
BF16 = jnp.bfloat16


def round_up(value, unit):
    return -(-value // unit) * unit


class Sizes:
    def __init__(self, ep, edp, tp, tok_rows, feats, hid):
        self.ep, self.edp, self.tp = ep, edp, tp
        self.window = ep // PARTS
        self.tok_rows, self.feats, self.hid = tok_rows, feats, hid
        self.block = feats * tp // edp
        self.nblk = feats // self.block
        self.sub = SUB if self.block % (SUB * 512) == 0 else 1
        self.piece = self.block // self.sub
        self.npc = feats // self.piece
        self.nch = max(1, min(4, self.piece // 128, max(2, self.piece // 256)))
        self.cw = self.piece // self.nch
        self.xr = round_up(2 * CAP * self.nch, 8)
        self.rows = round_up(ep * CAP, 16)
        self.lanes = round_up(3 * ep * CAP, 128)
        self.both = tp * hid
        side = math.isqrt(ep)
        side = side if side * side == ep else ep
        steps = [(a, b) for a in range(ep // side) for b in range(side) if a or b]
        self.side, self.steps = side, sorted(steps, key=lambda ab: -(bool(ab[0]) + bool(ab[1])))


def permutations(z):
    table = np.zeros((z.nch, 2, z.rows, z.ep, z.xr), np.float32)
    factor = np.zeros((z.nch, z.lanes, z.ep, z.xr), np.float32)
    place = np.zeros((3, z.rows, z.lanes), np.float32)
    for i in range(z.ep):
        for c in range(CAP):
            for q in range(z.nch):
                for a in range(2):
                    table[q, a, i * CAP + c, i, (2 * q + a) * CAP + c] = 1.0
                for m in range(3):
                    factor[q, (m * z.ep + i) * CAP + c, i, (2 * q + m // 2) * CAP + c] = 1.0
            for m in range(3):
                place[m, i * CAP + c, (m * z.ep + i) * CAP + c] = 1.0
    flat = table.reshape(z.nch * 2 * z.rows, z.ep * z.xr)
    return flat, flat.T.copy(), factor.reshape(-1, z.ep * z.xr), place


def slot_parts(index, nch):
    chunk = jnp.zeros_like(index)
    for k in range(1, nch):
        chunk += (index >= 2 * CAP * k).astype(jnp.int32)
    rest = index - 2 * CAP * chunk
    array = (rest >= CAP).astype(jnp.int32)
    return chunk, array, rest - CAP * array


def landed(ref, sem):
    pltpu.make_async_copy(ref, ref, sem).wait()


def kernel(
    z, tok_in, cot_in, ids_in, rw_in, perm_in, perm_t_in, factor_in, place_in, weights,
    wg, summed, homes,
    tok, cot, ids, rw, perm, perm_t, factor, place,
    wb, x, xin, zb, rb, rows, pout, pin, hgu, hh, hs, lb, ob, y, yin, right,
    in_sem, w_loc, w_send, w_recv, x_send, x_recv, z_send, z_recv, r_send, r_recv, p_send, p_recv,
    l_send, l_recv, y_send, y_recv, q_send, q_recv, upper,
):
    i, e, s = lax.axis_index("ep"), lax.axis_index("edp"), lax.axis_index("tp")
    barrier = pltpu.get_barrier_semaphore()
    down, across = i // z.side, lax.rem(i, z.side)
    peers = [
        lax.rem(down + a, z.ep // z.side) * z.side + lax.rem(across + b, z.side) for a, b in z.steps
    ]

    loads = [
        pltpu.make_async_copy(source, target, in_sem.at[k])
        for k, (source, target) in enumerate((
            (ids_in, ids), (rw_in, rw), (tok_in, tok), (cot_in, cot),
            (perm_in, perm), (perm_t_in, perm_t), (factor_in, factor), (place_in, place),
        ))
    ]
    for copy in loads[:4]:
        copy.start()

    for to in peers:
        pl.semaphore_signal(barrier, inc=1, device_id=(to, e, s), device_id_type=MESH)
    for d in range(1, z.tp):
        pl.semaphore_signal(barrier, inc=1, device_id=(i, e, lax.rem(s + d, z.tp)), device_id_type=MESH)
    for d in range(1, z.edp):
        @pl.when(e + d < z.edp)
        def _():
            pl.semaphore_signal(barrier, inc=1, device_id=(i, e + d, s), device_id_type=MESH)

    own_w = pltpu.make_async_copy(
        weights.at[:, :, pl.ds(pl.multiple_of(s * z.feats, 128), z.feats)], wb.at[:, s], w_loc
    )
    own_w.start()
    for copy in loads[4:]:
        copy.start()

    row = lax.broadcasted_iota(jnp.int32, (z.xr, z.tok_rows), 0)
    chunk, array, slot = slot_parts(row, z.nch)
    in_use = row < 2 * CAP * z.nch
    before = (
        lax.broadcasted_iota(jnp.int32, (z.tok_rows, z.tok_rows), 0)
        < lax.broadcasted_iota(jnp.int32, (z.tok_rows, z.tok_rows), 1)
    ).astype(F32).astype(BF16)
    lane = lax.broadcasted_iota(jnp.int32, (z.tok_rows, z.xr), 1)
    lane_chunk, lane_array, _ = slot_parts(lane, z.nch)
    loads[0].wait()
    loads[1].wait()
    ids_t = ids[...]
    rw_t = rw[...]
    chosen, scales, picks = [], [], []
    for w in range(z.window):
        hit = (ids_t == w).astype(F32)
        match = jnp.sum(hit, axis=0, keepdims=True)
        weight = jnp.sum(hit * rw_t, axis=0, keepdims=True)
        match_all = jnp.broadcast_to(match, (z.xr, z.tok_rows))
        rank = jnp.dot(match_all.astype(BF16), before, preferred_element_type=F32)
        pick = jnp.where(in_use & (rank == slot.astype(F32)), match_all, 0.0)
        slot_weight = jnp.sum(pick * weight, axis=1, keepdims=True)
        picks.append(pick)
        scales.append((
            jnp.where(array[:, :1] == 1, slot_weight, 1.0), jnp.where(array[:, :1] == 0, slot_weight, 1.0),
        ))
        chosen.append([
            [jnp.where((chunk == q) & (array == a), pick, 0.0).astype(BF16) for a in range(2)]
            for q in range(z.nch)
        ])
    loads[2].wait()
    loads[3].wait()

    def gather(p):
        for w in range(z.window):
            total = jnp.zeros((z.xr, z.cw), F32)
            for q in range(z.nch):
                cols = pl.ds(p * z.piece + q * z.cw, z.cw)
                for a, source in ((0, tok), (1, cot)):
                    total += jnp.dot(chosen[w][q][a], source[:, cols], preferred_element_type=F32)
            x[w, p] = (total * scales[w][0]).astype(BF16)

    sent = []

    def send(source, target, send_sem, recv_sem, to):
        sent.append(pltpu.make_async_remote_copy(
            src_ref=source, dst_ref=target, send_sem=send_sem, recv_sem=recv_sem,
            device_id=to, device_id_type=MESH,
        ))
        sent[-1].start()

    for p in range(z.npc):
        gather(p)
        if p == 0:
            pl.semaphore_wait(barrier, z.ep - 1 + z.tp - 1 + e)
        for k, to in enumerate(peers):
            send(
                x.at[to // PARTS, p], xin.at[i, p],
                x_send.at[k * z.npc + p], x_recv.at[i * z.npc + p], (to, e, s),
            )
        if p == 0:
            for b in range(z.nblk):
                for d in range(1, z.tp):
                    to = lax.rem(s + d, z.tp)
                    cols = pl.ds(pl.multiple_of(to * z.feats + b * z.block, 128), z.block)
                    send(
                        weights.at[:, :, cols], wb.at[:, s, :, pl.ds(b * z.block, z.block)],
                        w_send.at[d * z.nblk + b], w_recv.at[s * z.nblk + b], (i, e, to),
                    )
    for d in range(1, z.edp):
        @pl.when(e - d >= 0)
        def _():
            pl.semaphore_signal(upper, inc=1, device_id=(i, e - d, s), device_id_type=MESH)

    for p in range(z.npc):
        xin[i, p] = x[i // PARTS, p]
    for w in range(z.window):
        home = jnp.transpose(picks[w])
        for q in range(z.nch):
            for a in range(2):
                homes[w, 2 * q + a] = jnp.where(
                    (lane_chunk == q) & (lane_array == a), home, 0.0
                ).astype(BF16)

    def replica_copy(b):
        to = s * z.nblk + b
        slot_at = lax.rem(e - to + z.edp, z.edp) - 1
        return pltpu.make_async_remote_copy(
            src_ref=x.at[:, pl.ds(b * z.sub, z.sub)], dst_ref=zb.at[slot_at],
            send_sem=z_send.at[b], recv_sem=z_recv.at[slot_at],
            device_id=(i, to, s), device_id_type=MESH,
        )

    @pl.when(e < z.edp - 1)
    def _():
        pl.semaphore_wait(upper, z.edp - 1 - e)

    for b in range(z.nblk):
        @pl.when(s * z.nblk + b != e)
        def _():
            replica_copy(b).start()

    own_w.wait()
    for copy in loads[4:]:
        copy.wait()

    owner = e // z.nblk
    mine = e - owner * z.nblk
    last = (((1,), (1,)), ((), ()))
    gu, dh = pl.ds(0, 2 * z.both), pl.ds(2 * z.both, z.both)
    for p in range(z.npc):
        for to in peers:
            landed(xin.at[to, p], x_recv.at[to * z.npc + p])
        flat = jnp.dot(
            perm[...], xin[:, p].reshape(z.ep * z.xr, z.cw), preferred_element_type=F32
        ).astype(BF16)
        for q in range(z.nch):
            rows[:, q * z.cw:(q + 1) * z.cw] = flat[q * 2 * z.rows:(q + 1) * 2 * z.rows]
        if p % z.sub == 0:
            b = p // z.sub
            for d in range(1, z.tp):
                source = lax.rem(s + d, z.tp)
                landed(wb.at[:, source, :, pl.ds(b * z.block, z.block)], w_recv.at[source * z.nblk + b])
        cols = pl.ds(p * z.piece, z.piece)
        for part, which, at in ((rows[:z.rows], pl.ds(0, 2), gu), (rows[z.rows:], pl.ds(2, 1), dh)):
            value = lax.dot_general(
                part, wb[which, :, :, cols].reshape(-1, z.piece), last, preferred_element_type=F32
            )
            if p:
                value += pout[:, at]
            pout[:, at] = value
            if p == z.npc - 1:
                for d in range(1, z.tp):
                    k = 0 if at is gu else 1
                    send(
                        pout.at[:, at], pin.at[s, :, at],
                        p_send.at[d * 2 + k], p_recv.at[s * 2 + k], (i, e, lax.rem(s + d, z.tp)),
                    )

    def spread_copy(k, to):
        return pltpu.make_async_remote_copy(
            src_ref=zb.at[:, to // PARTS], dst_ref=rb.at[pl.ds(1, z.edp - 1), i],
            send_sem=r_send.at[k], recv_sem=r_recv.at[i],
            device_id=(to, e, s), device_id_type=MESH,
        )

    @pl.when(s == owner)
    def _():
        for d in range(1, z.edp):
            landed(zb.at[d - 1], z_recv.at[d - 1])
        for k, to in enumerate(peers):
            spread_copy(k, to).start()

    for d in range(1, z.tp):
        source = lax.rem(s + d, z.tp)
        for k, at in enumerate((gu, dh)):
            landed(pin.at[source, :, at], p_recv.at[source * 2 + k])

    sums = pout[...]
    for d in range(1, z.tp):
        sums += pin[lax.rem(s + d, z.tp)]
    gate, up, d_hidden = (sums[:, m * z.both:(m + 1) * z.both] for m in range(3))
    sig = jax.nn.sigmoid(gate)
    active = gate * sig
    hh[...] = (active * up).astype(BF16)
    hgu[:, :z.both] = (d_hidden * up * sig * (1.0 + gate * (1.0 - sig))).astype(BF16)
    hgu[:, z.both:] = (d_hidden * active).astype(BF16)

    def output(p):
        cols = pl.ds(p * z.piece, z.piece)
        out = jnp.dot(hh[...], wb[2, :, :, cols].reshape(-1, z.piece), preferred_element_type=F32)
        back = jnp.dot(hgu[...], wb[:2, :, :, cols].reshape(-1, z.piece), preferred_element_type=F32)
        for q in range(z.nch):
            for a, value in enumerate((out, back)):
                at = (2 * q + a) * z.rows
                ob[at:at + z.rows] = value[:, q * z.cw:(q + 1) * z.cw].astype(BF16)
        total = jnp.dot(perm_t[...], ob[...], preferred_element_type=F32)
        y[:, p] = total.astype(BF16).reshape(z.ep, z.xr, z.cw)
        for k, to in enumerate(peers):
            send(
                y.at[to, p], yin.at[i, p],
                y_send.at[k * z.npc + p], y_recv.at[i * z.npc + p], (to, e, s),
            )

    first = (((0,), (0,)), ((), ()))
    output(0)
    for t in range(z.tp):
        at = slice(t * z.hid, (t + 1) * z.hid)
        hs[t, 0] = hgu[:, at]
        hs[t, 1] = hgu[:, z.both + t * z.hid:z.both + (t + 1) * z.hid]
        hs[t, 2] = hh[:, at]
    packed = jnp.zeros((z.hid, z.lanes), F32)
    for m in range(3):
        packed += lax.dot_general(hs[s, m], place[m], first, preferred_element_type=F32)
    lb[0] = packed.astype(BF16)
    upward = (2 * e) // z.edp
    for k in range(z.edp - 1):
        low = k + (k - e + z.edp) // z.edp
        high = z.edp - 1 - k
        high = high - (e - high + z.edp) // z.edp
        to = upward * low + (1 - upward) * high
        slot_at = lax.rem(e - to + z.edp, z.edp)
        send(lb.at[0], lb.at[slot_at], l_send.at[k], l_recv.at[slot_at], (i, to, s))
    for p in range(1, z.npc):
        output(p)
    yin[i] = y[i]

    def relay(d):
        return pltpu.make_async_remote_copy(
            src_ref=rb, dst_ref=rb, send_sem=q_send.at[d], recv_sem=q_recv.at[0],
            device_id=(i, e, lax.rem(s + d, z.tp)), device_id_type=MESH,
        )

    @pl.when(s == owner)
    def _():
        for p in range(z.sub):
            rb[0, :, p] = xin[:, mine * z.sub + p]
        rb[1:, i] = zb[:, i // PARTS]
        for to in peers:
            landed(rb.at[pl.ds(1, z.edp - 1), to], r_recv.at[to])
        for d in range(1, z.tp):
            relay(d).start()

    @pl.when(s != owner)
    def _():
        landed(rb, q_recv.at[0])

    for r in range(z.edp):
        for p in range(z.sub):
            flat = jnp.dot(
                factor[...], rb[r, :, p].reshape(z.ep * z.xr, z.cw), preferred_element_type=F32
            ).astype(BF16)
            for q in range(z.nch):
                right[pl.ds(r * z.lanes, z.lanes), pl.ds(p * z.piece + q * z.cw, z.cw)] = flat[
                    q * z.lanes:(q + 1) * z.lanes
                ]

    for p in range(z.npc):
        for to in peers:
            landed(yin.at[to, p], y_recv.at[to * z.npc + p])
        for w in range(z.window):
            total = yin[w * PARTS, p].astype(F32)
            for h in range(1, PARTS):
                total += yin[w * PARTS + h, p].astype(F32)
            summed[w, p] = (total * scales[w][1]).astype(BF16)

    for d in range(1, z.edp):
        landed(lb.at[d], l_recv.at[d])
    lane = lax.broadcasted_iota(jnp.int32, (1, z.lanes), 1)
    width = z.ep * CAP
    for m in range(3):
        keep = ((lane >= m * width) & (lane < (m + 1) * width)).astype(F32).astype(BF16)
        factors = jnp.concatenate([lb[r] * keep for r in range(z.edp)], axis=1)
        wg[m] = jnp.dot(factors, right[...], preferred_element_type=F32)

    for copy in sent:
        copy.wait_send()
    for b in range(z.nblk):
        @pl.when(s * z.nblk + b != e)
        def _():
            replica_copy(b).wait_send()

    @pl.when(s == owner)
    def _():
        for k, to in enumerate(peers):
            spread_copy(k, to).wait_send()
        for d in range(1, z.tp):
            relay(d).wait_send()


def finish(z, wg, summed, homes, mixed, grad_tok, wgrad, mix, grad, sem):
    copies = []
    for m in range(3):
        copies.append(pltpu.make_async_copy(wg.at[m], wgrad.at[m], sem.at[m]))
        copies[-1].start()
    for p in range(z.npc):
        value = jnp.zeros((2 * z.nch * z.tok_rows, z.cw), F32)
        for w in range(z.window):
            home = homes[w].reshape(2 * z.nch * z.tok_rows, z.xr)
            value += jnp.dot(home, summed[w, p], preferred_element_type=F32)
        for q in range(z.nch):
            cols = pl.ds(p * z.piece + q * z.cw, z.cw)
            for a, target in ((0, mix), (1, grad)):
                at = (2 * q + a) * z.tok_rows
                target[:, cols] = value[at:at + z.tok_rows].astype(BF16)
    for a, target in ((0, mix), (1, grad)):
        copies.append(pltpu.make_async_copy(target, (mixed, grad_tok)[a], sem.at[3 + a]))
        copies[-1].start()
    for copy in copies:
        copy.wait()


def shards(tokens, cotangent, expert_ids, route_weights, expert_weights):
    z = Sizes(
        lax.axis_size("ep"), lax.axis_size("edp"), lax.axis_size("tp"),
        tokens.shape[0], tokens.shape[1], expert_weights.shape[1],
    )
    tables = [jnp.asarray(table, BF16) for table in permutations(z)]
    operands = [tokens, cotangent, expert_ids.T, route_weights.T] + tables
    hbm = pl.BlockSpec(memory_space=pltpu.HBM)
    vmem = pl.BlockSpec(memory_space=pltpu.VMEM)
    dma = pltpu.SemaphoreType.DMA
    passed = pl.pallas_call(
        functools.partial(kernel, z),
        out_shape=(
            pltpu.VMEM((3, z.hid, z.block), F32),
            pltpu.VMEM((z.window, z.npc, z.xr, z.cw), BF16),
            pltpu.VMEM((z.window, 2 * z.nch, z.tok_rows, z.xr), BF16),
        ),
        in_specs=[hbm] * (len(operands) + 1),
        out_specs=(vmem,) * 3,
        scratch_shapes=[pltpu.VMEM(o.shape, o.dtype) for o in operands] + [
            pltpu.VMEM((3, z.tp, z.hid, z.feats), BF16),
            pltpu.VMEM((z.window, z.npc, z.xr, z.cw), BF16),
            pltpu.VMEM((z.ep, z.npc, z.xr, z.cw), BF16),
            pltpu.VMEM((z.edp - 1, z.window, z.sub, z.xr, z.cw), BF16),
            pltpu.VMEM((z.edp, z.ep, z.sub, z.xr, z.cw), BF16),
            pltpu.VMEM((2 * z.rows, z.piece), BF16),
            pltpu.VMEM((z.rows, 3 * z.both), F32),
            pltpu.VMEM((z.tp, z.rows, 3 * z.both), F32),
            pltpu.VMEM((z.rows, 2 * z.both), BF16),
            pltpu.VMEM((z.rows, z.both), BF16),
            pltpu.VMEM((z.tp, 3, z.rows, z.hid), BF16),
            pltpu.VMEM((z.edp, z.hid, z.lanes), BF16),
            pltpu.VMEM((z.nch * 2 * z.rows, z.cw), BF16),
            pltpu.VMEM((z.ep, z.npc, z.xr, z.cw), BF16),
            pltpu.VMEM((z.ep, z.npc, z.xr, z.cw), BF16),
            pltpu.VMEM((z.edp * z.lanes, z.block), BF16),
        ] + [
            dma((len(operands),)), dma, dma((z.tp * z.nblk,)), dma((z.tp * z.nblk,)),
            dma((z.ep * z.npc,)), dma((z.ep * z.npc,)),
            dma((z.nblk,)), dma((z.edp - 1,)), dma((z.ep,)), dma((z.ep,)),
            dma((z.tp * 2,)), dma((z.tp * 2,)),
            dma((z.edp,)), dma((z.edp,)), dma((z.ep * z.npc,)), dma((z.ep * z.npc,)),
            dma((z.tp,)), dma((1,)), pltpu.SemaphoreType.REGULAR,
        ],
        compiler_params=pltpu.CompilerParams(
            collective_id=0, has_side_effects=True, vmem_limit_bytes=VMEM_LIMIT
        ),
        name="expert_block",
    )(*[pltpu.with_memory_space_constraint(o, pltpu.HBM) for o in (*operands, expert_weights)])
    return pl.pallas_call(
        functools.partial(finish, z),
        out_shape=(
            jax.ShapeDtypeStruct(tokens.shape, BF16),
            jax.ShapeDtypeStruct(tokens.shape, BF16),
            jax.ShapeDtypeStruct((3, z.hid, z.block), F32),
        ),
        in_specs=[vmem] * 3,
        out_specs=(hbm,) * 3,
        scratch_shapes=[
            pltpu.VMEM(tokens.shape, BF16),
            pltpu.VMEM(tokens.shape, BF16),
            dma((5,)),
        ],
        compiler_params=pltpu.CompilerParams(vmem_limit_bytes=VMEM_LIMIT),
        name="finish",
    )(*[pltpu.with_memory_space_constraint(o, pltpu.VMEM) for o in passed])


def solution(mesh):
    placed = (
        P(("ep", "edp"), "tp"),
        P(("ep", "edp"), "tp"),
        P(("ep", "edp"), None),
        P(("ep", "edp"), None),
        P(None, ("ep", "tp"), None),
    )
    return jax.shard_map(
        shards,
        mesh=mesh,
        in_specs=placed,
        out_specs=(P(("ep", "edp"), "tp"), P(("ep", "edp"), "tp"), P(None, ("ep", "tp"), "edp")),
        check_vma=False,
    )
```

```python
import functools
import math

import jax
import jax.numpy as jnp
import numpy as np
from jax import lax
from jax.experimental import pallas as pl
from jax.experimental.pallas import tpu as pltpu
from jax.sharding import PartitionSpec as P

CAP = 10
PARTS = 4
SUB = 2
VMEM_LIMIT = 40 * 1024 * 1024
MESH = pl.DeviceIdType.MESH
F32 = jnp.float32
BF16 = jnp.bfloat16


def round_up(value, unit):
    return -(-value // unit) * unit


class Sizes:
    def __init__(self, ep, edp, tp, tok_rows, feats, hid):
        self.ep, self.edp, self.tp = ep, edp, tp
        self.window = ep // PARTS
        self.tok_rows, self.feats, self.hid = tok_rows, feats, hid
        self.block = feats * tp // edp
        self.nblk = feats // self.block
        self.sub = SUB if self.block % (SUB * 512) == 0 else 1
        self.piece = self.block // self.sub
        self.npc = feats // self.piece
        self.nch = max(1, min(4, self.piece // 128, max(2, self.piece // 256)))
        self.cw = self.piece // self.nch
        self.xr = round_up(2 * CAP * self.nch, 8)
        self.rows = round_up(ep * CAP, 16)
        self.lanes = round_up(3 * ep * CAP, 128)
        self.both = tp * hid
        wide, tall = ep * self.xr, self.nch * 2 * self.rows
        self.tables, at = [], 0
        for n, width in ((tall, wide), (wide, tall), (self.nch * self.lanes, wide), (3 * self.rows, self.lanes)):
            self.tables.append((at, n, width))
            at += n
        self.table_lanes = round_up(max(width for _, _, width in self.tables), 128)
        side = math.isqrt(ep)
        side = side if side * side == ep else ep
        steps = [(a, b) for a in range(ep // side) for b in range(side) if a or b]
        self.side, self.steps = side, sorted(steps, key=lambda ab: -(bool(ab[0]) + bool(ab[1])))


def permutations(z):
    table = np.zeros((z.nch, 2, z.rows, z.ep, z.xr), np.float32)
    factor = np.zeros((z.nch, z.lanes, z.ep, z.xr), np.float32)
    place = np.zeros((3, z.rows, z.lanes), np.float32)
    for i in range(z.ep):
        for c in range(CAP):
            for q in range(z.nch):
                for a in range(2):
                    table[q, a, i * CAP + c, i, (2 * q + a) * CAP + c] = 1.0
                for m in range(3):
                    factor[q, (m * z.ep + i) * CAP + c, i, (2 * q + m // 2) * CAP + c] = 1.0
            for m in range(3):
                place[m, i * CAP + c, (m * z.ep + i) * CAP + c] = 1.0
    flat = table.reshape(z.nch * 2 * z.rows, z.ep * z.xr)
    packed = np.zeros((sum(n for _, n, _ in z.tables), z.table_lanes), np.float32)
    for (at, n, width), part in zip(z.tables, (flat, flat.T, factor, place), strict=True):
        packed[at:at + n, :width] = part.reshape(n, width)
    return packed


def slot_parts(index, nch):
    chunk = jnp.zeros_like(index)
    for k in range(1, nch):
        chunk += (index >= 2 * CAP * k).astype(jnp.int32)
    rest = index - 2 * CAP * chunk
    array = (rest >= CAP).astype(jnp.int32)
    return chunk, array, rest - CAP * array


def landed(ref, sem):
    pltpu.make_async_copy(ref, ref, sem).wait()


def kernel(
    z, tok_in, cot_in, ids_in, rw_in, tables_in, weights,
    wg, summed, homes,
    data, ids, rw, tables,
    wb, x, xin, zb, rb, rows, pout, pin, hgu, hh, hs, lb, ob, y, yin, right,
    in_sem, w_loc, w_send, w_recv, x_send, x_recv, z_send, z_recv, r_send, r_recv, p_send, p_recv,
    l_send, l_recv, y_send, y_recv, q_send, q_recv, ep_ready, edp_ready, tp_ready,
):
    i, e, s = lax.axis_index("ep"), lax.axis_index("edp"), lax.axis_index("tp")
    barrier = pltpu.get_barrier_semaphore()
    down, across = i // z.side, lax.rem(i, z.side)
    peers = [
        lax.rem(down + a, z.ep // z.side) * z.side + lax.rem(across + b, z.side) for a, b in z.steps
    ]
    partners = [lax.rem(s + d, z.tp) for d in range(1, z.tp)]
    perm, perm_t, factor, place = (tables.at[pl.ds(at, n), pl.ds(0, width)] for at, n, width in z.tables)

    loads = [
        pltpu.make_async_copy(ids_in, ids, in_sem.at[0]),
        pltpu.make_async_copy(rw_in, rw, in_sem.at[1]),
        pltpu.make_async_copy(tok_in, data.at[0], in_sem.at[2]),
        pltpu.make_async_copy(cot_in, data.at[1], in_sem.at[2]),
    ]
    for copy in loads:
        copy.start()

    def signal(semaphore, condition, to):
        @pl.when(condition)
        def _():
            pl.semaphore_signal(semaphore, inc=1, device_id=to, device_id_type=MESH)

    for to in partners:
        signal(barrier, to > s, (i, e, to))
    for to in peers:
        signal(barrier, to > i, (to, e, s))
    for d in range(1, z.edp):
        signal(barrier, e + d < z.edp, (i, lax.rem(e + d, z.edp), s))

    @pl.when(i + e + s > 0)
    def _():
        pl.semaphore_wait(barrier, i + e + s)

    for to in partners:
        signal(tp_ready, to < s, (i, e, to))
    for to in peers:
        signal(ep_ready.at[i], to < i, (to, e, s))
    for d in range(1, z.edp):
        signal(edp_ready, e - d >= 0, (i, lax.rem(e - d + z.edp, z.edp), s))

    @pl.when(s < z.tp - 1)
    def _():
        pl.semaphore_wait(tp_ready, z.tp - 1 - s)

    def send(source, target, send_sem, recv_sem, to):
        pltpu.make_async_remote_copy(
            src_ref=source, dst_ref=target, send_sem=send_sem, recv_sem=recv_sem,
            device_id=to, device_id_type=MESH,
        ).start()

    for b in range(z.nblk):
        for to in partners:
            cols = pl.ds(pl.multiple_of(to * z.feats + b * z.block, 128), z.block)
            send(
                weights.at[:, :, cols], wb.at[:, s, :, pl.ds(b * z.block, z.block)],
                w_send, w_recv.at[b], (i, e, to),
            )

    row = lax.broadcasted_iota(jnp.int32, (z.xr, z.tok_rows), 0)
    chunk, array, slot = slot_parts(row, z.nch)
    in_use = row < 2 * CAP * z.nch
    before = (
        lax.broadcasted_iota(jnp.int32, (z.tok_rows, z.tok_rows), 0)
        < lax.broadcasted_iota(jnp.int32, (z.tok_rows, z.tok_rows), 1)
    ).astype(F32).astype(BF16)
    lane = lax.broadcasted_iota(jnp.int32, (z.tok_rows, z.xr), 1)
    lane_chunk, lane_array, _ = slot_parts(lane, z.nch)
    loads[0].wait()
    loads[1].wait()
    ids_t = ids[...]
    rw_t = rw[...]
    chosen, scales, picks = [], [], []
    for w in range(z.window):
        hit = (ids_t == w).astype(F32)
        match = jnp.sum(hit, axis=0, keepdims=True)
        weight = jnp.sum(hit * rw_t, axis=0, keepdims=True)
        match_all = jnp.broadcast_to(match, (z.xr, z.tok_rows))
        rank = jnp.dot(match_all.astype(BF16), before, preferred_element_type=F32)
        pick = jnp.where(in_use & (rank == slot.astype(F32)), match_all, 0.0)
        slot_weight = jnp.sum(pick * weight, axis=1, keepdims=True)
        picks.append(pick)
        scales.append((
            jnp.where(array[:, :1] == 1, slot_weight, 1.0), jnp.where(array[:, :1] == 0, slot_weight, 1.0),
        ))
        chosen.append([
            [jnp.where((chunk == q) & (array == a), pick, 0.0).astype(BF16) for a in range(2)]
            for q in range(z.nch)
        ])
    landed(data, in_sem.at[2])
    own_w = pltpu.make_async_copy(
        weights.at[:, :, pl.ds(pl.multiple_of(s * z.feats, 128), z.feats)], wb.at[:, s], w_loc
    )
    own_w.start()
    table_load = pltpu.make_async_copy(tables_in, tables, in_sem.at[3])
    table_load.start()

    def send_rows(p, to):
        send(x.at[to // PARTS, p], xin.at[i, p], x_send, x_recv.at[p], (to, e, s))

    def send_replica(b):
        to = s * z.nblk + b
        slot_at = lax.rem(e - to + z.edp, z.edp) - 1
        send(x.at[:, pl.ds(b * z.sub, z.sub)], zb.at[slot_at], z_send, z_recv, (i, to, s))

    for p in range(z.npc):
        for w in range(z.window):
            total = jnp.zeros((z.xr, z.cw), F32)
            for q in range(z.nch):
                cols = pl.ds(p * z.piece + q * z.cw, z.cw)
                for a in range(2):
                    total += jnp.dot(chosen[w][q][a], data[a, :, cols], preferred_element_type=F32)
            x[w, p] = (total * scales[w][0]).astype(BF16)
        for to in peers:
            @pl.when(to < i)
            def _():
                send_rows(p, to)
    for to in reversed(peers):
        @pl.when(to > i)
        def _():
            pl.semaphore_wait(ep_ready.at[to], 1)
            for p in range(z.npc):
                send_rows(p, to)
    for b in range(z.nblk):
        @pl.when(s * z.nblk + b < e)
        def _():
            send_replica(b)

    for p in range(z.npc):
        xin[i, p] = x[i // PARTS, p]
    for w in range(z.window):
        home = jnp.transpose(picks[w])
        for q in range(z.nch):
            for a in range(2):
                homes[w, 2 * q + a] = jnp.where(
                    (lane_chunk == q) & (lane_array == a), home, 0.0
                ).astype(BF16)
    own_w.wait()
    table_load.wait()

    owner = e // z.nblk
    mine = e - owner * z.nblk
    last = (((1,), (1,)), ((), ()))
    for p in range(z.npc):
        landed(xin.at[pl.ds(0, z.ep - 1), p], x_recv.at[p])
        if p == 0:
            @pl.when(e < z.edp - 1)
            def _():
                pl.semaphore_wait(edp_ready, z.edp - 1 - e)

            for b in range(z.nblk):
                @pl.when(s * z.nblk + b > e)
                def _():
                    send_replica(b)
        flat = jnp.dot(
            perm[...], xin[:, p].reshape(z.ep * z.xr, z.cw), preferred_element_type=F32
        ).astype(BF16)
        for q in range(z.nch):
            rows[:, q * z.cw:(q + 1) * z.cw] = flat[q * 2 * z.rows:(q + 1) * 2 * z.rows]
        if p % z.sub == 0:
            b = p // z.sub
            landed(wb.at[:, pl.ds(0, z.tp - 1), :, pl.ds(b * z.block, z.block)], w_recv.at[b])
        cols = pl.ds(p * z.piece, z.piece)
        first_two = lax.dot_general(
            rows[:z.rows], wb[:2, :, :, cols].reshape(-1, z.piece), last, preferred_element_type=F32
        )
        third = lax.dot_general(
            rows[z.rows:], wb[2, :, :, cols].reshape(-1, z.piece), last, preferred_element_type=F32
        )
        if p:
            first_two += pout[:, :2 * z.both]
            third += pout[:, 2 * z.both:]
        pout[:, :2 * z.both] = first_two
        pout[:, 2 * z.both:] = third
    for to in partners:
        send(pout, pin.at[s], p_send, p_recv, (i, e, to))

    others = pl.ds(1, z.edp - 1)

    @pl.when(s == owner)
    def _():
        landed(zb, z_recv)
        for to in peers:
            send(zb.at[:, to // PARTS], rb.at[others, i], r_send, r_recv.at[i], (to, e, s))
        for k, to in enumerate(partners):
            send(
                xin.at[:, pl.ds(mine * z.sub, z.sub)], rb.at[0], q_send.at[k], q_recv, (i, e, to),
            )
            send(zb.at[:, i // PARTS], rb.at[others, i], q_send.at[k], q_recv, (i, e, to))

    landed(pin.at[pl.ds(0, z.tp - 1)], p_recv)
    sums = pout[...]
    for source in partners:
        sums += pin[source]
    gate, up, d_hidden = (sums[:, m * z.both:(m + 1) * z.both] for m in range(3))
    sig = jax.nn.sigmoid(gate)
    active = gate * sig
    hh[...] = (active * up).astype(BF16)
    hgu[:, :z.both] = (d_hidden * up * sig * (1.0 + gate * (1.0 - sig))).astype(BF16)
    hgu[:, z.both:] = (d_hidden * active).astype(BF16)

    def output(p):
        cols = pl.ds(p * z.piece, z.piece)
        out = jnp.dot(hh[...], wb[2, :, :, cols].reshape(-1, z.piece), preferred_element_type=F32)
        back = jnp.dot(hgu[...], wb[:2, :, :, cols].reshape(-1, z.piece), preferred_element_type=F32)
        for q in range(z.nch):
            for a, value in enumerate((out, back)):
                at = (2 * q + a) * z.rows
                ob[at:at + z.rows] = value[:, q * z.cw:(q + 1) * z.cw].astype(BF16)
        total = jnp.dot(perm_t[...], ob[...], preferred_element_type=F32)
        y[:, p] = total.astype(BF16).reshape(z.ep, z.xr, z.cw)
        for to in peers:
            send(y.at[to, p], yin.at[i, p], y_send, y_recv.at[p], (to, e, s))

    first = (((0,), (0,)), ((), ()))
    output(0)
    for t in range(z.tp):
        at = slice(t * z.hid, (t + 1) * z.hid)
        hs[t, 0] = hgu[:, at]
        hs[t, 1] = hgu[:, z.both + t * z.hid:z.both + (t + 1) * z.hid]
        hs[t, 2] = hh[:, at]
    packed = jnp.zeros((z.hid, z.lanes), F32)
    for m in range(3):
        packed += lax.dot_general(
            hs[s, m], place[m * z.rows:(m + 1) * z.rows], first, preferred_element_type=F32
        )
    lb[0] = packed.astype(BF16)
    upward = (2 * e) // z.edp
    for k in range(z.edp - 1):
        low = k + (k - e + z.edp) // z.edp
        high = z.edp - 1 - k
        high = high - (e - high + z.edp) // z.edp
        to = upward * low + (1 - upward) * high
        slot_at = lax.rem(e - to + z.edp, z.edp)
        send(lb.at[0], lb.at[slot_at], l_send, l_recv.at[slot_at], (i, to, s))
    for p in range(1, z.npc):
        output(p)
    yin[i] = y[i]

    @pl.when(s == owner)
    def _():
        for p in range(z.sub):
            rb[0, :, p] = xin[:, mine * z.sub + p]
        rb[1:, i] = zb[:, i // PARTS]
        for to in peers:
            landed(rb.at[others, to], r_recv.at[to])
            for k, core in enumerate(partners):
                send(rb.at[others, to], rb.at[others, to], q_send.at[k], q_recv, (i, e, core))

    @pl.when(s != owner)
    def _():
        landed(rb, q_recv)

    for r in range(z.edp):
        for p in range(z.sub):
            flat = jnp.dot(
                factor[...], rb[r, :, p].reshape(z.ep * z.xr, z.cw), preferred_element_type=F32
            ).astype(BF16)
            for q in range(z.nch):
                right[pl.ds(r * z.lanes, z.lanes), pl.ds(p * z.piece + q * z.cw, z.cw)] = flat[
                    q * z.lanes:(q + 1) * z.lanes
                ]
    for d in range(1, z.edp):
        landed(lb.at[d], l_recv.at[d])
    lane = lax.broadcasted_iota(jnp.int32, (1, z.lanes), 1)
    width = z.ep * CAP
    for m in range(3):
        keep = ((lane >= m * width) & (lane < (m + 1) * width)).astype(F32).astype(BF16)
        factors = jnp.concatenate([lb[r] * keep for r in range(z.edp)], axis=1)
        wg[m] = jnp.dot(factors, right[...], preferred_element_type=F32)

    for p in range(z.npc):
        landed(yin.at[pl.ds(0, z.ep - 1), p], y_recv.at[p])
        for w in range(z.window):
            total = yin[w * PARTS, p].astype(F32)
            for h in range(1, PARTS):
                total += yin[w * PARTS + h, p].astype(F32)
            summed[w, p] = (total * scales[w][1]).astype(BF16)

    landed(wb.at[:, pl.ds(0, z.tp - 1)], w_send)
    landed(xin.at[pl.ds(0, z.ep - 1)], x_send)
    landed(yin.at[pl.ds(0, z.ep - 1)], y_send)
    landed(pin.at[pl.ds(0, z.tp - 1)], p_send)
    landed(lb.at[others], l_send)

    @pl.when(s == owner)
    def _():
        if z.nblk > 1:
            landed(x.at[:, pl.ds(0, (z.nblk - 1) * z.sub)], z_send)
        landed(rb.at[others, pl.ds(0, z.ep - 1)], r_send)
        for k in range(z.tp - 1):
            landed(rb, q_send.at[k])

    @pl.when(s != owner)
    def _():
        landed(x, z_send)


def finish(z, wg, summed, homes, mixed, grad_tok, wgrad, mix, grad, sem):
    copies = []
    for m in range(3):
        copies.append(pltpu.make_async_copy(wg.at[m], wgrad.at[m], sem.at[m]))
        copies[-1].start()
    for p in range(z.npc):
        value = jnp.zeros((2 * z.nch * z.tok_rows, z.cw), F32)
        for w in range(z.window):
            home = homes[w].reshape(2 * z.nch * z.tok_rows, z.xr)
            value += jnp.dot(home, summed[w, p], preferred_element_type=F32)
        for q in range(z.nch):
            cols = pl.ds(p * z.piece + q * z.cw, z.cw)
            for a, target in ((0, mix), (1, grad)):
                at = (2 * q + a) * z.tok_rows
                target[:, cols] = value[at:at + z.tok_rows].astype(BF16)
    for a, target in ((0, mix), (1, grad)):
        copies.append(pltpu.make_async_copy(target, (mixed, grad_tok)[a], sem.at[3 + a]))
        copies[-1].start()
    for copy in copies:
        copy.wait()


def shards(tokens, cotangent, expert_ids, route_weights, expert_weights):
    z = Sizes(
        lax.axis_size("ep"), lax.axis_size("edp"), lax.axis_size("tp"),
        tokens.shape[0], tokens.shape[1], expert_weights.shape[1],
    )
    tables = jnp.asarray(permutations(z), BF16)
    operands = [tokens, cotangent, expert_ids.T, route_weights.T, tables, expert_weights]
    hbm = pl.BlockSpec(memory_space=pltpu.HBM)
    vmem = pl.BlockSpec(memory_space=pltpu.VMEM)
    dma = pltpu.SemaphoreType.DMA
    passed = pl.pallas_call(
        functools.partial(kernel, z),
        out_shape=(
            pltpu.VMEM((3, z.hid, z.block), F32),
            pltpu.VMEM((z.window, z.npc, z.xr, z.cw), BF16),
            pltpu.VMEM((z.window, 2 * z.nch, z.tok_rows, z.xr), BF16),
        ),
        in_specs=[hbm] * len(operands),
        out_specs=(vmem,) * 3,
        scratch_shapes=[
            pltpu.VMEM((2, *tokens.shape), BF16),
            *(pltpu.VMEM(o.shape, o.dtype) for o in operands[2:5]),
            pltpu.VMEM((3, z.tp, z.hid, z.feats), BF16),
            pltpu.VMEM((z.window, z.npc, z.xr, z.cw), BF16),
            pltpu.VMEM((z.ep, z.npc, z.xr, z.cw), BF16),
            pltpu.VMEM((z.edp - 1, z.window, z.sub, z.xr, z.cw), BF16),
            pltpu.VMEM((z.edp, z.ep, z.sub, z.xr, z.cw), BF16),
            pltpu.VMEM((2 * z.rows, z.piece), BF16),
            pltpu.VMEM((z.rows, 3 * z.both), F32),
            pltpu.VMEM((z.tp, z.rows, 3 * z.both), F32),
            pltpu.VMEM((z.rows, 2 * z.both), BF16),
            pltpu.VMEM((z.rows, z.both), BF16),
            pltpu.VMEM((z.tp, 3, z.rows, z.hid), BF16),
            pltpu.VMEM((z.edp, z.hid, z.lanes), BF16),
            pltpu.VMEM((z.nch * 2 * z.rows, z.cw), BF16),
            pltpu.VMEM((z.ep, z.npc, z.xr, z.cw), BF16),
            pltpu.VMEM((z.ep, z.npc, z.xr, z.cw), BF16),
            pltpu.VMEM((z.edp * z.lanes, z.block), BF16),
            dma((4,)), dma, dma, dma((z.nblk,)), dma, dma((z.npc,)), dma, dma, dma, dma((z.ep,)), dma, dma,
            dma, dma((z.edp,)), dma, dma((z.npc,)), dma((z.tp - 1,)), dma,
            pltpu.SemaphoreType.REGULAR((z.ep,)), pltpu.SemaphoreType.REGULAR, pltpu.SemaphoreType.REGULAR,
        ],
        compiler_params=pltpu.CompilerParams(
            collective_id=0, has_side_effects=True, vmem_limit_bytes=VMEM_LIMIT
        ),
        name="expert_block",
    )(*[pltpu.with_memory_space_constraint(o, pltpu.HBM) for o in operands])
    return pl.pallas_call(
        functools.partial(finish, z),
        out_shape=(
            jax.ShapeDtypeStruct(tokens.shape, BF16),
            jax.ShapeDtypeStruct(tokens.shape, BF16),
            jax.ShapeDtypeStruct((3, z.hid, z.block), F32),
        ),
        in_specs=[vmem] * 3,
        out_specs=(hbm,) * 3,
        scratch_shapes=[
            pltpu.VMEM(tokens.shape, BF16),
            pltpu.VMEM(tokens.shape, BF16),
            dma((5,)),
        ],
        compiler_params=pltpu.CompilerParams(vmem_limit_bytes=VMEM_LIMIT),
        name="finish",
    )(*[pltpu.with_memory_space_constraint(o, pltpu.VMEM) for o in passed])


def solution(mesh):
    placed = (
        P(("ep", "edp"), "tp"),
        P(("ep", "edp"), "tp"),
        P(("ep", "edp"), None),
        P(("ep", "edp"), None),
        P(None, ("ep", "tp"), None),
    )
    return jax.shard_map(
        shards,
        mesh=mesh,
        in_specs=placed,
        out_specs=(P(("ep", "edp"), "tp"), P(("ep", "edp"), "tp"), P(None, ("ep", "tp"), "edp")),
        check_vma=False,
    )
```

```python
import functools
import math

import jax
import jax.numpy as jnp
import numpy as np
from jax import lax
from jax.experimental import pallas as pl
from jax.experimental.pallas import tpu as pltpu
from jax.sharding import PartitionSpec as P

CAP = 10
PARTS = 4
SUB = 2
VMEM_LIMIT = 40 * 1024 * 1024
MESH = pl.DeviceIdType.MESH
F32 = jnp.float32
BF16 = jnp.bfloat16


def round_up(value, unit):
    return -(-value // unit) * unit


class Sizes:
    def __init__(self, ep, edp, tp, tok_rows, feats, hid):
        self.ep, self.edp, self.tp = ep, edp, tp
        self.window = ep // PARTS
        self.tok_rows, self.feats, self.hid = tok_rows, feats, hid
        self.block = feats * tp // edp
        self.nblk = feats // self.block
        self.sub = SUB if self.block % (SUB * 512) == 0 else 1
        self.piece = self.block // self.sub
        self.npc = feats // self.piece
        self.nch = max(1, min(4, self.piece // 128, max(2, self.piece // 256)))
        self.cw = self.piece // self.nch
        self.xr = round_up(2 * CAP * self.nch, 8)
        self.rows = round_up(ep * CAP, 16)
        self.lanes = round_up(3 * ep * CAP, 128)
        self.both = tp * hid
        wide, tall = ep * self.xr, self.nch * 2 * self.rows
        self.tables, at = [], 0
        for n, width in ((tall, wide), (wide, tall), (self.nch * self.lanes, wide), (3 * self.rows, self.lanes)):
            self.tables.append((at, n, width))
            at += n
        self.table_lanes = round_up(max(width for _, _, width in self.tables), 128)
        side = math.isqrt(ep)
        side = side if side * side == ep else ep
        steps = [(a, b) for a in range(ep // side) for b in range(side) if a or b]
        self.side, self.steps = side, sorted(steps, key=lambda ab: -(bool(ab[0]) + bool(ab[1])))


def permutations(z):
    table = np.zeros((z.nch, 2, z.rows, z.ep, z.xr), np.float32)
    factor = np.zeros((z.nch, z.lanes, z.ep, z.xr), np.float32)
    place = np.zeros((3, z.rows, z.lanes), np.float32)
    for i in range(z.ep):
        for c in range(CAP):
            for q in range(z.nch):
                for a in range(2):
                    table[q, a, i * CAP + c, i, (2 * q + a) * CAP + c] = 1.0
                for m in range(3):
                    factor[q, (m * z.ep + i) * CAP + c, i, (2 * q + m // 2) * CAP + c] = 1.0
            for m in range(3):
                place[m, i * CAP + c, (m * z.ep + i) * CAP + c] = 1.0
    flat = table.reshape(z.nch * 2 * z.rows, z.ep * z.xr)
    packed = np.zeros((sum(n for _, n, _ in z.tables), z.table_lanes), np.float32)
    for (at, n, width), part in zip(z.tables, (flat, flat.T, factor, place), strict=True):
        packed[at:at + n, :width] = part.reshape(n, width)
    return packed


def slot_parts(index, nch):
    chunk = jnp.zeros_like(index)
    for k in range(1, nch):
        chunk += (index >= 2 * CAP * k).astype(jnp.int32)
    rest = index - 2 * CAP * chunk
    array = (rest >= CAP).astype(jnp.int32)
    return chunk, array, rest - CAP * array


def landed(ref, sem):
    pltpu.make_async_copy(ref, ref, sem).wait()


def kernel(
    z, tok_in, cot_in, ids_in, rw_in, tables_in, weights,
    wg, summed, homes,
    data, ids, rw, tables,
    wb, x, xin, zb, rb, rows, pout, pwire, pin, hgu, hh, hs, lb, ob, y, yin, right,
    in_sem, w_loc, w_send, w_recv, x_send, x_recv, z_send, z_recv, r_send, r_recv, p_send, p_recv,
    l_send, l_recv, y_send, y_recv, q_send, q_recv, core_ready, plane_ready, edp_ready,
):
    i, e, s = lax.axis_index("ep"), lax.axis_index("edp"), lax.axis_index("tp")
    barrier = pltpu.get_barrier_semaphore()
    down, across = i // z.side, lax.rem(i, z.side)
    peers = [
        lax.rem(down + a, z.ep // z.side) * z.side + lax.rem(across + b, z.side) for a, b in z.steps
    ]
    partners = [lax.rem(s + d, z.tp) for d in range(1, z.tp)]
    perm, perm_t, factor, place = (tables.at[pl.ds(at, n), pl.ds(0, width)] for at, n, width in z.tables)

    loads = [
        pltpu.make_async_copy(ids_in, ids, in_sem.at[0]),
        pltpu.make_async_copy(rw_in, rw, in_sem.at[1]),
    ]
    head, rest = pl.ds(0, z.piece), pl.ds(z.piece, z.feats - z.piece)
    for k, cols in enumerate((head, rest)):
        loads.append(pltpu.make_async_copy(tok_in.at[:, cols], data.at[0, :, cols], in_sem.at[2 + k]))
        loads.append(pltpu.make_async_copy(cot_in.at[:, cols], data.at[1, :, cols], in_sem.at[2 + k]))
    for copy in loads:
        copy.start()

    def signal(semaphore, to):
        pl.semaphore_signal(semaphore, inc=1, device_id=to, device_id_type=MESH)

    last_core = z.tp - 1
    lead = s == last_core
    @pl.when(lead)
    def _():
        for t in range(last_core):
            signal(barrier, (i, e, t))

    for to in peers:
        signal(barrier, (to, e, last_core))
    for d in range(1, z.edp):
        @pl.when(e + d < z.edp)
        def _():
            signal(barrier, (i, lax.rem(e + d, z.edp), 0))

    @pl.when(s == 0)
    def _():
        pl.semaphore_wait(barrier, 1 + e * z.tp)

    @pl.when((s != 0) & (s != last_core))
    def _():
        pl.semaphore_wait(barrier, 1)

    @pl.when(s != last_core)
    def _():
        signal(core_ready, (i, e, last_core))
        if z.tp > 2:
            pl.semaphore_wait(core_ready, 1)

    @pl.when(lead)
    def _():
        pl.semaphore_wait(core_ready, last_core)
        if z.tp > 2:
            for t in range(last_core):
                signal(core_ready, (i, e, t))

    @pl.when(s == 0)
    def _():
        for d in range(1, z.edp):
            @pl.when(e - d >= 0)
            def _():
                for t in range(z.tp):
                    signal(edp_ready, (i, lax.rem(e - d + z.edp, z.edp), t))

    def enter():
        @pl.when(lead)
        def _():
            pl.semaphore_wait(barrier, (z.ep - 1) * z.tp)
            for t in range(last_core):
                signal(plane_ready, (i, e, t))

        @pl.when(s != last_core)
        def _():
            pl.semaphore_wait(plane_ready, 1)

    def send(source, target, send_sem, recv_sem, to):
        pltpu.make_async_remote_copy(
            src_ref=source, dst_ref=target, send_sem=send_sem, recv_sem=recv_sem,
            device_id=to, device_id_type=MESH,
        ).start()

    for b in range(z.nblk):
        for to in partners:
            cols = pl.ds(pl.multiple_of(to * z.feats + b * z.block, 128), z.block)
            send(
                weights.at[:, :, cols], wb.at[:, s, :, pl.ds(b * z.block, z.block)],
                w_send, w_recv.at[b], (i, e, to),
            )

    row = lax.broadcasted_iota(jnp.int32, (z.xr, z.tok_rows), 0)
    chunk, array, slot = slot_parts(row, z.nch)
    in_use = row < 2 * CAP * z.nch
    before = (
        lax.broadcasted_iota(jnp.int32, (z.tok_rows, z.tok_rows), 0)
        < lax.broadcasted_iota(jnp.int32, (z.tok_rows, z.tok_rows), 1)
    ).astype(F32).astype(BF16)
    lane = lax.broadcasted_iota(jnp.int32, (z.tok_rows, z.xr), 1)
    lane_chunk, lane_array, _ = slot_parts(lane, z.nch)
    loads[0].wait()
    loads[1].wait()
    ids_t = ids[...]
    rw_t = rw[...]
    chosen, scales, picks = [], [], []
    for w in range(z.window):
        hit = (ids_t == w).astype(F32)
        match = jnp.sum(hit, axis=0, keepdims=True)
        weight = jnp.sum(hit * rw_t, axis=0, keepdims=True)
        match_all = jnp.broadcast_to(match, (z.xr, z.tok_rows))
        rank = jnp.dot(match_all.astype(BF16), before, preferred_element_type=F32)
        pick = jnp.where(in_use & (rank == slot.astype(F32)), match_all, 0.0)
        slot_weight = jnp.sum(pick * weight, axis=1, keepdims=True)
        picks.append(pick)
        scales.append((
            jnp.where(array[:, :1] == 1, slot_weight, 1.0), jnp.where(array[:, :1] == 0, slot_weight, 1.0),
        ))
        chosen.append([
            [jnp.where((chunk == q) & (array == a), pick, 0.0).astype(BF16) for a in range(2)]
            for q in range(z.nch)
        ])
    landed(data.at[:, :, head], in_sem.at[2])
    own_w = pltpu.make_async_copy(
        weights.at[:, :, pl.ds(pl.multiple_of(s * z.feats, 128), z.feats)], wb.at[:, s], w_loc
    )
    table_load = pltpu.make_async_copy(tables_in, tables, in_sem.at[4])

    def send_rows(p, to):
        send(x.at[to // PARTS, p], xin.at[i, p], x_send, x_recv.at[p], (to, e, s))

    def send_replica(b):
        to = s * z.nblk + b
        slot_at = lax.rem(e - to + z.edp, z.edp) - 1
        send(x.at[:, pl.ds(b * z.sub, z.sub)], zb.at[slot_at], z_send, z_recv, (i, to, s))

    for p in range(z.npc):
        if p == 1:
            landed(data.at[:, :, rest], in_sem.at[3])
            own_w.start()
            table_load.start()
        for w in range(z.window):
            total = jnp.zeros((z.xr, z.cw), F32)
            for q in range(z.nch):
                cols = pl.ds(p * z.piece + q * z.cw, z.cw)
                for a in range(2):
                    total += jnp.dot(chosen[w][q][a], data[a, :, cols], preferred_element_type=F32)
            x[w, p] = (total * scales[w][0]).astype(BF16)
        if p % z.sub == z.sub - 1:
            @pl.when(s * z.nblk + p // z.sub < e)
            def _():
                send_replica(p // z.sub)

    enter()

    def send_all():
        for p in range(z.npc):
            for to in peers:
                send_rows(p, to)

    early = lax.rem(s, 2) == 0

    @pl.when(early)
    def _():
        send_all()

    for p in range(z.npc):
        xin[i, p] = x[i // PARTS, p]
    for w in range(z.window):
        home = jnp.transpose(picks[w])
        for q in range(z.nch):
            for a in range(2):
                homes[w, 2 * q + a] = jnp.where(
                    (lane_chunk == q) & (lane_array == a), home, 0.0
                ).astype(BF16)

    @pl.when(~early)
    def _():
        send_all()

    @pl.when(e < z.edp - 1)
    def _():
        pl.semaphore_wait(edp_ready, z.edp - 1 - e)

    for b in range(z.nblk):
        @pl.when(s * z.nblk + b > e)
        def _():
            send_replica(b)
    own_w.wait()
    table_load.wait()

    owner = e // z.nblk
    mine = e - owner * z.nblk
    last = (((1,), (1,)), ((), ()))

    def unpack(p):
        flat = jnp.dot(
            perm[...], xin[:, p].reshape(z.ep * z.xr, z.cw), preferred_element_type=F32
        ).astype(BF16)
        for q in range(z.nch):
            rows[p % 2, :, q * z.cw:(q + 1) * z.cw] = flat[q * 2 * z.rows:(q + 1) * 2 * z.rows]

    def wait_piece(p):
        landed(xin.at[pl.ds(0, z.ep - 1), p], x_recv.at[p])

    def wait_weights(p):
        if p % z.sub == 0:
            b = p // z.sub
            landed(wb.at[:, pl.ds(0, z.tp - 1), :, pl.ds(b * z.block, z.block)], w_recv.at[b])

    def project(p):
        cols = pl.ds(p * z.piece, z.piece)
        first_two = lax.dot_general(
            rows[p % 2, :z.rows], wb[:2, :, :, cols].reshape(-1, z.piece), last, preferred_element_type=F32
        )
        third = lax.dot_general(
            rows[p % 2, z.rows:], wb[2, :, :, cols].reshape(-1, z.piece), last, preferred_element_type=F32
        )
        if p:
            first_two += pout[:, :2 * z.both]
            third += pout[:, 2 * z.both:]
        pout[:, :2 * z.both] = first_two
        pout[:, 2 * z.both:] = third
        if p == z.npc - 1:
            pwire[:, :2 * z.both] = first_two.astype(BF16)
            pwire[:, 2 * z.both:] = third.astype(BF16)

    wait_piece(0)
    unpack(0)
    others = pl.ds(1, z.edp - 1)

    def spread():
        @pl.when(s == owner)
        def _():
            landed(zb, z_recv)
            for to in peers:
                send(zb.at[:, to // PARTS], rb.at[others, i], r_send, r_recv.at[i], (to, e, s))
            for k, to in enumerate(partners):
                send(zb.at[:, i // PARTS], rb.at[others, i], q_send.at[k], q_recv, (i, e, to))

    for p in range(1, z.npc):
        if p == 2:
            spread()
        if p < z.npc - 1:
            wait_piece(p)
        wait_weights(p - 1)
        if p < z.npc - 1:
            unpack(p)
        project(p - 1)
    wait_piece(z.npc - 1)
    wait_weights(z.npc - 1)
    unpack(z.npc - 1)
    project(z.npc - 1)
    for to in partners:
        send(pwire, pin.at[s], p_send, p_recv, (i, e, to))

    @pl.when(s == owner)
    def _():
        for k, to in enumerate(partners):
            send(xin.at[:, pl.ds(mine * z.sub, z.sub)], rb.at[0], q_send.at[k], q_recv, (i, e, to))


    landed(pin.at[pl.ds(0, z.tp - 1)], p_recv)
    sums = pout[...]
    for source in partners:
        sums += pin[source].astype(F32)
    gate, up, d_hidden = (sums[:, m * z.both:(m + 1) * z.both] for m in range(3))
    sig = jax.nn.sigmoid(gate)
    active = gate * sig
    hh[...] = (active * up).astype(BF16)
    hgu[:, :z.both] = (d_hidden * up * sig * (1.0 + gate * (1.0 - sig))).astype(BF16)
    hgu[:, z.both:] = (d_hidden * active).astype(BF16)

    def output(p):
        cols = pl.ds(p * z.piece, z.piece)
        out = jnp.dot(hh[...], wb[2, :, :, cols].reshape(-1, z.piece), preferred_element_type=F32)
        back = jnp.dot(hgu[...], wb[:2, :, :, cols].reshape(-1, z.piece), preferred_element_type=F32)
        for q in range(z.nch):
            for a, value in enumerate((out, back)):
                at = (2 * q + a) * z.rows
                ob[at:at + z.rows] = value[:, q * z.cw:(q + 1) * z.cw].astype(BF16)
        total = jnp.dot(perm_t[...], ob[...], preferred_element_type=F32)
        y[:, p] = total.astype(BF16).reshape(z.ep, z.xr, z.cw)
        for to in peers:
            send(y.at[to, p], yin.at[i, p], y_send, y_recv.at[p], (to, e, s))

    first = (((0,), (0,)), ((), ()))
    def factors_out():
        for t in range(z.tp):
            at = slice(t * z.hid, (t + 1) * z.hid)
            hs[t, :z.rows] = hgu[:, at]
            hs[t, z.rows:2 * z.rows] = hgu[:, z.both + t * z.hid:z.both + (t + 1) * z.hid]
            hs[t, 2 * z.rows:] = hh[:, at]
        lb[0] = lax.dot_general(hs[s], place[...], first, preferred_element_type=F32).astype(BF16)
        upward = (2 * e) // z.edp
        for k in range(z.edp - 1):
            low = k + (k - e + z.edp) // z.edp
            high = z.edp - 1 - k
            high = high - (e - high + z.edp) // z.edp
            to = upward * low + (1 - upward) * high
            slot_at = lax.rem(e - to + z.edp, z.edp)
            send(lb.at[0], lb.at[slot_at], l_send, l_recv.at[slot_at], (i, to, s))

    factors_first = (2 * e) // z.edp + lax.rem(s, 2) > 0
    @pl.when(factors_first)
    def _():
        factors_out()
    output(0)
    @pl.when(~factors_first)
    def _():
        factors_out()
    for p in range(1, z.npc):
        output(p)
    yin[i] = y[i]

    @pl.when(s == owner)
    def _():
        for p in range(z.sub):
            rb[0, :, p] = xin[:, mine * z.sub + p]
        rb[1:, i] = zb[:, i // PARTS]
        for to in peers:
            landed(rb.at[others, to], r_recv.at[to])
            for k, core in enumerate(partners):
                send(rb.at[others, to], rb.at[others, to], q_send.at[k], q_recv, (i, e, core))

    @pl.when(s != owner)
    def _():
        landed(rb, q_recv)

    for r in range(z.edp):
        for p in range(z.sub):
            flat = jnp.dot(
                factor[...], rb[r, :, p].reshape(z.ep * z.xr, z.cw), preferred_element_type=F32
            ).astype(BF16)
            for q in range(z.nch):
                right[pl.ds(r * z.lanes, z.lanes), pl.ds(p * z.piece + q * z.cw, z.cw)] = flat[
                    q * z.lanes:(q + 1) * z.lanes
                ]
    lane = lax.broadcasted_iota(jnp.int32, (1, z.lanes), 1)
    width = z.ep * CAP
    keeps = [((lane >= m * width) & (lane < (m + 1) * width)).astype(F32).astype(BF16) for m in range(3)]
    near = max(1, z.edp // 2)
    for part in (range(near), range(near, z.edp)):
        for d in part:
            if d:
                landed(lb.at[d], l_recv.at[d])
        for m in range(3):
            factors = jnp.concatenate([lb[d] * keeps[m] for d in part], axis=1)
            value = jnp.dot(
                factors, right[part.start * z.lanes:part.stop * z.lanes], preferred_element_type=F32
            )
            if part.start:
                value += wg[m]
            wg[m] = value

    for p in range(z.npc):
        landed(yin.at[pl.ds(0, z.ep - 1), p], y_recv.at[p])
        for w in range(z.window):
            total = yin[w * PARTS, p].astype(F32)
            for h in range(1, PARTS):
                total += yin[w * PARTS + h, p].astype(F32)
            summed[w, p] = (total * scales[w][1]).astype(BF16)

    landed(wb.at[:, pl.ds(0, z.tp - 1)], w_send)
    landed(xin.at[pl.ds(0, z.ep - 1)], x_send)
    landed(yin.at[pl.ds(0, z.ep - 1)], y_send)
    landed(pin.at[pl.ds(0, z.tp - 1)], p_send)
    landed(lb.at[others], l_send)

    @pl.when(s == owner)
    def _():
        if z.nblk > 1:
            landed(x.at[:, pl.ds(0, (z.nblk - 1) * z.sub)], z_send)
        landed(rb.at[others, pl.ds(0, z.ep - 1)], r_send)
        for k in range(z.tp - 1):
            landed(rb, q_send.at[k])

    @pl.when(s != owner)
    def _():
        landed(x, z_send)


def finish(z, wg, summed, homes, mixed, grad_tok, wgrad, mix, grad, sem):
    copies = []
    for m in range(3):
        copies.append(pltpu.make_async_copy(wg.at[m], wgrad.at[m], sem.at[m]))
        copies[-1].start()
    for p in range(z.npc):
        value = jnp.zeros((2 * z.nch * z.tok_rows, z.cw), F32)
        for w in range(z.window):
            home = homes[w].reshape(2 * z.nch * z.tok_rows, z.xr)
            value += jnp.dot(home, summed[w, p], preferred_element_type=F32)
        for q in range(z.nch):
            cols = pl.ds(p * z.piece + q * z.cw, z.cw)
            for a, target in ((0, mix), (1, grad)):
                at = (2 * q + a) * z.tok_rows
                target[:, cols] = value[at:at + z.tok_rows].astype(BF16)
    for a, target in ((0, mix), (1, grad)):
        copies.append(pltpu.make_async_copy(target, (mixed, grad_tok)[a], sem.at[3 + a]))
        copies[-1].start()
    for copy in copies:
        copy.wait()


def shards(tokens, cotangent, expert_ids, route_weights, expert_weights):
    z = Sizes(
        lax.axis_size("ep"), lax.axis_size("edp"), lax.axis_size("tp"),
        tokens.shape[0], tokens.shape[1], expert_weights.shape[1],
    )
    tables = jnp.asarray(permutations(z), BF16)
    operands = [tokens, cotangent, expert_ids.T, route_weights.T, tables, expert_weights]
    hbm = pl.BlockSpec(memory_space=pltpu.HBM)
    vmem = pl.BlockSpec(memory_space=pltpu.VMEM)
    dma = pltpu.SemaphoreType.DMA
    passed = pl.pallas_call(
        functools.partial(kernel, z),
        out_shape=(
            pltpu.VMEM((3, z.hid, z.block), F32),
            pltpu.VMEM((z.window, z.npc, z.xr, z.cw), BF16),
            pltpu.VMEM((z.window, 2 * z.nch, z.tok_rows, z.xr), BF16),
        ),
        in_specs=[hbm] * len(operands),
        out_specs=(vmem,) * 3,
        scratch_shapes=[
            pltpu.VMEM((2, *tokens.shape), BF16),
            *(pltpu.VMEM(o.shape, o.dtype) for o in operands[2:5]),
            pltpu.VMEM((3, z.tp, z.hid, z.feats), BF16),
            pltpu.VMEM((z.window, z.npc, z.xr, z.cw), BF16),
            pltpu.VMEM((z.ep, z.npc, z.xr, z.cw), BF16),
            pltpu.VMEM((z.edp - 1, z.window, z.sub, z.xr, z.cw), BF16),
            pltpu.VMEM((z.edp, z.ep, z.sub, z.xr, z.cw), BF16),
            pltpu.VMEM((2, 2 * z.rows, z.piece), BF16),
            pltpu.VMEM((z.rows, 3 * z.both), F32),
            pltpu.VMEM((z.rows, 3 * z.both), BF16),
            pltpu.VMEM((z.tp, z.rows, 3 * z.both), BF16),
            pltpu.VMEM((z.rows, 2 * z.both), BF16),
            pltpu.VMEM((z.rows, z.both), BF16),
            pltpu.VMEM((z.tp, 3 * z.rows, z.hid), BF16),
            pltpu.VMEM((z.edp, z.hid, z.lanes), BF16),
            pltpu.VMEM((z.nch * 2 * z.rows, z.cw), BF16),
            pltpu.VMEM((z.ep, z.npc, z.xr, z.cw), BF16),
            pltpu.VMEM((z.ep, z.npc, z.xr, z.cw), BF16),
            pltpu.VMEM((z.edp * z.lanes, z.block), BF16),
            dma((5,)), dma, dma, dma((z.nblk,)), dma, dma((z.npc,)), dma, dma, dma, dma((z.ep,)), dma, dma,
            dma, dma((z.edp,)), dma, dma((z.npc,)), dma((z.tp - 1,)), dma,
            pltpu.SemaphoreType.REGULAR, pltpu.SemaphoreType.REGULAR, pltpu.SemaphoreType.REGULAR,
        ],
        compiler_params=pltpu.CompilerParams(
            collective_id=0, has_side_effects=True, vmem_limit_bytes=VMEM_LIMIT
        ),
        name="expert_block",
    )(*[pltpu.with_memory_space_constraint(o, pltpu.HBM) for o in operands])
    return pl.pallas_call(
        functools.partial(finish, z),
        out_shape=(
            jax.ShapeDtypeStruct(tokens.shape, BF16),
            jax.ShapeDtypeStruct(tokens.shape, BF16),
            jax.ShapeDtypeStruct((3, z.hid, z.block), F32),
        ),
        in_specs=[vmem] * 3,
        out_specs=(hbm,) * 3,
        scratch_shapes=[
            pltpu.VMEM(tokens.shape, BF16),
            pltpu.VMEM(tokens.shape, BF16),
            dma((5,)),
        ],
        compiler_params=pltpu.CompilerParams(vmem_limit_bytes=VMEM_LIMIT),
        name="finish",
    )(*[pltpu.with_memory_space_constraint(o, pltpu.VMEM) for o in passed])


def solution(mesh):
    placed = (
        P(("ep", "edp"), "tp"),
        P(("ep", "edp"), "tp"),
        P(("ep", "edp"), None),
        P(("ep", "edp"), None),
        P(None, ("ep", "tp"), None),
    )
    return jax.shard_map(
        shards,
        mesh=mesh,
        in_specs=placed,
        out_specs=(P(("ep", "edp"), "tp"), P(("ep", "edp"), "tp"), P(None, ("ep", "tp"), "edp")),
        check_vma=False,
    )
```

```python
import functools
import math

import jax
import jax.numpy as jnp
import numpy as np
from jax import lax
from jax.experimental import pallas as pl
from jax.experimental.pallas import tpu as pltpu
from jax.sharding import PartitionSpec as P

CAP = 10
PARTS = 4
SUB = 2
VMEM_LIMIT = 40 * 1024 * 1024
MESH = pl.DeviceIdType.MESH
F32 = jnp.float32
BF16 = jnp.bfloat16


def round_up(value, unit):
    return -(-value // unit) * unit


class Sizes:
    def __init__(self, ep, edp, tp, tok_rows, feats, hid):
        self.ep, self.edp, self.tp = ep, edp, tp
        self.window = ep // PARTS
        self.tok_rows, self.feats, self.hid = tok_rows, feats, hid
        self.block = feats * tp // edp
        self.nblk = feats // self.block
        self.sub = SUB if self.block % (SUB * 512) == 0 else 1
        self.piece = self.block // self.sub
        self.npc = feats // self.piece
        self.nch = max(1, min(4, self.piece // 128, max(2, self.piece // 256)))
        self.cw = self.piece // self.nch
        self.xr = round_up(2 * CAP * self.nch, 8)
        self.rows = round_up(ep * CAP, 16)
        self.lanes = round_up(3 * ep * CAP, 128)
        self.both = tp * hid
        wide, tall = ep * self.xr, self.nch * 2 * self.rows
        self.tables, at = [], 0
        for n, width in ((tall, wide), (wide, tall), (self.nch * self.lanes, wide), (3 * self.rows, self.lanes)):
            self.tables.append((at, n, width))
            at += n
        self.table_lanes = round_up(max(width for _, _, width in self.tables), 128)
        side = math.isqrt(ep)
        side = side if side * side == ep else ep
        steps = [(a, b) for a in range(ep // side) for b in range(side) if a or b]
        self.side, self.steps = side, sorted(steps, key=lambda ab: -(bool(ab[0]) + bool(ab[1])))


def permutations(z):
    table = np.zeros((z.nch, 2, z.rows, z.ep, z.xr), np.float32)
    factor = np.zeros((z.nch, z.lanes, z.ep, z.xr), np.float32)
    place = np.zeros((3, z.rows, z.lanes), np.float32)
    for i in range(z.ep):
        for c in range(CAP):
            for q in range(z.nch):
                for a in range(2):
                    table[q, a, i * CAP + c, i, (2 * q + a) * CAP + c] = 1.0
                for m in range(3):
                    factor[q, (m * z.ep + i) * CAP + c, i, (2 * q + m // 2) * CAP + c] = 1.0
            for m in range(3):
                place[m, i * CAP + c, (m * z.ep + i) * CAP + c] = 1.0
    flat = table.reshape(z.nch * 2 * z.rows, z.ep * z.xr)
    packed = np.zeros((sum(n for _, n, _ in z.tables), z.table_lanes), np.float32)
    for (at, n, width), part in zip(z.tables, (flat, flat.T, factor, place), strict=True):
        packed[at:at + n, :width] = part.reshape(n, width)
    return packed


def slot_parts(index, nch):
    chunk = jnp.zeros_like(index)
    for k in range(1, nch):
        chunk += (index >= 2 * CAP * k).astype(jnp.int32)
    rest = index - 2 * CAP * chunk
    array = (rest >= CAP).astype(jnp.int32)
    return chunk, array, rest - CAP * array


def landed(ref, sem):
    pltpu.make_async_copy(ref, ref, sem).wait()


def kernel(
    z, tok_in, cot_in, ids_in, rw_in, tables_in, weights,
    wg, summed, homes,
    data, ids, rw, tables,
    wb, x, xin, zb, rb, rows, pout, pwire, pin, hgu, hh, hs, lb, ob, y, yin, right,
    in_sem, w_loc, w_send, w_recv, x_send, x_recv, z_send, z_recv, r_send, r_recv, p_send, p_recv,
    l_send, l_recv, y_send, y_recv, q_send, q_recv, core_ready, plane_ready, edp_ready,
):
    i, e, s = lax.axis_index("ep"), lax.axis_index("edp"), lax.axis_index("tp")
    barrier = pltpu.get_barrier_semaphore()
    down, across = i // z.side, lax.rem(i, z.side)
    peers = [
        lax.rem(down + a, z.ep // z.side) * z.side + lax.rem(across + b, z.side) for a, b in z.steps
    ]
    partners = [lax.rem(s + d, z.tp) for d in range(1, z.tp)]
    perm, perm_t, factor, place = (tables.at[pl.ds(at, n), pl.ds(0, width)] for at, n, width in z.tables)

    loads = [
        pltpu.make_async_copy(ids_in, ids, in_sem.at[0]),
        pltpu.make_async_copy(rw_in, rw, in_sem.at[1]),
    ]
    head, rest = pl.ds(0, z.piece), pl.ds(z.piece, z.feats - z.piece)
    for k, cols in enumerate((head, rest)):
        loads.append(pltpu.make_async_copy(tok_in.at[:, cols], data.at[0, :, cols], in_sem.at[2 + k]))
        loads.append(pltpu.make_async_copy(cot_in.at[:, cols], data.at[1, :, cols], in_sem.at[2 + k]))
    for copy in loads:
        copy.start()

    def signal(semaphore, to):
        pl.semaphore_signal(semaphore, inc=1, device_id=to, device_id_type=MESH)

    last_core = z.tp - 1
    lead = s == last_core
    @pl.when(lead)
    def _():
        for t in range(last_core):
            signal(barrier, (i, e, t))

    for to in peers:
        signal(barrier, (to, e, last_core))
    for d in range(1, z.edp):
        @pl.when(e + d < z.edp)
        def _():
            signal(barrier, (i, lax.rem(e + d, z.edp), 0))

    @pl.when(s == 0)
    def _():
        pl.semaphore_wait(barrier, 1 + e * z.tp)

    @pl.when((s != 0) & (s != last_core))
    def _():
        pl.semaphore_wait(barrier, 1)

    @pl.when(s != last_core)
    def _():
        signal(core_ready, (i, e, last_core))
        if z.tp > 2:
            pl.semaphore_wait(core_ready, 1)

    @pl.when(lead)
    def _():
        pl.semaphore_wait(core_ready, last_core)
        if z.tp > 2:
            for t in range(last_core):
                signal(core_ready, (i, e, t))

    @pl.when(s == 0)
    def _():
        for d in range(1, z.edp):
            @pl.when(e - d >= 0)
            def _():
                for t in range(z.tp):
                    signal(edp_ready, (i, lax.rem(e - d + z.edp, z.edp), t))

    def enter():
        @pl.when(lead)
        def _():
            pl.semaphore_wait(barrier, (z.ep - 1) * z.tp)
            for t in range(last_core):
                signal(plane_ready, (i, e, t))

        @pl.when(s != last_core)
        def _():
            pl.semaphore_wait(plane_ready, 1)

    def send(source, target, send_sem, recv_sem, to):
        pltpu.make_async_remote_copy(
            src_ref=source, dst_ref=target, send_sem=send_sem, recv_sem=recv_sem,
            device_id=to, device_id_type=MESH,
        ).start()

    for b in range(z.nblk):
        for to in partners:
            cols = pl.ds(pl.multiple_of(to * z.feats + b * z.block, 128), z.block)
            send(
                weights.at[:, :, cols], wb.at[:, s, :, pl.ds(b * z.block, z.block)],
                w_send, w_recv.at[b], (i, e, to),
            )

    row = lax.broadcasted_iota(jnp.int32, (z.xr, z.tok_rows), 0)
    chunk, array, slot = slot_parts(row, z.nch)
    in_use = row < 2 * CAP * z.nch
    before = (
        lax.broadcasted_iota(jnp.int32, (z.tok_rows, z.tok_rows), 0)
        < lax.broadcasted_iota(jnp.int32, (z.tok_rows, z.tok_rows), 1)
    ).astype(F32).astype(BF16)
    lane = lax.broadcasted_iota(jnp.int32, (z.tok_rows, z.xr), 1)
    lane_chunk, lane_array, _ = slot_parts(lane, z.nch)
    loads[0].wait()
    loads[1].wait()
    ids_t = ids[...]
    rw_t = rw[...]
    chosen, scales, picks = [], [], []
    for w in range(z.window):
        hit = (ids_t == w).astype(F32)
        match = jnp.sum(hit, axis=0, keepdims=True)
        weight = jnp.sum(hit * rw_t, axis=0, keepdims=True)
        match_all = jnp.broadcast_to(match, (z.xr, z.tok_rows))
        rank = jnp.dot(match_all.astype(BF16), before, preferred_element_type=F32)
        pick = jnp.where(in_use & (rank == slot.astype(F32)), match_all, 0.0)
        slot_weight = jnp.sum(pick * weight, axis=1, keepdims=True)
        picks.append(pick)
        scales.append((
            jnp.where(array[:, :1] == 1, slot_weight, 1.0), jnp.where(array[:, :1] == 0, slot_weight, 1.0),
        ))
        chosen.append([
            [jnp.where((chunk == q) & (array == a), pick, 0.0).astype(BF16) for a in range(2)]
            for q in range(z.nch)
        ])
    landed(data.at[:, :, head], in_sem.at[2])
    own_w = pltpu.make_async_copy(
        weights.at[:, :, pl.ds(pl.multiple_of(s * z.feats, 128), z.feats)], wb.at[:, s], w_loc
    )
    table_load = pltpu.make_async_copy(tables_in, tables, in_sem.at[4])

    def send_rows(p, to):
        send(x.at[to // PARTS, p], xin.at[i, p], x_send, x_recv.at[p], (to, e, s))

    def send_replica(b):
        to = s * z.nblk + b
        slot_at = lax.rem(e - to + z.edp, z.edp) - 1
        send(x.at[:, pl.ds(b * z.sub, z.sub)], zb.at[slot_at], z_send, z_recv, (i, to, s))

    for p in range(z.npc):
        if p == 1:
            landed(data.at[:, :, rest], in_sem.at[3])
            own_w.start()
            table_load.start()
        for w in range(z.window):
            total = jnp.zeros((z.xr, z.cw), F32)
            for q in range(z.nch):
                cols = pl.ds(p * z.piece + q * z.cw, z.cw)
                for a in range(2):
                    total += jnp.dot(chosen[w][q][a], data[a, :, cols], preferred_element_type=F32)
            x[w, p] = (total * scales[w][0]).astype(BF16)
        if p % z.sub == z.sub - 1:
            @pl.when(s * z.nblk + p // z.sub < e)
            def _():
                send_replica(p // z.sub)

    enter()

    def send_all():
        for p in range(z.npc):
            for to in peers:
                send_rows(p, to)

    early = lax.rem(s, 2) == 0

    @pl.when(early)
    def _():
        send_all()

    for p in range(z.npc):
        xin[i, p] = x[i // PARTS, p]
    for w in range(z.window):
        home = jnp.transpose(picks[w])
        for q in range(z.nch):
            for a in range(2):
                homes[w, 2 * q + a] = jnp.where(
                    (lane_chunk == q) & (lane_array == a), home, 0.0
                ).astype(BF16)

    @pl.when(~early)
    def _():
        send_all()

    @pl.when(e < z.edp - 1)
    def _():
        pl.semaphore_wait(edp_ready, z.edp - 1 - e)

    for b in range(z.nblk):
        @pl.when(s * z.nblk + b > e)
        def _():
            send_replica(b)
    own_w.wait()
    table_load.wait()

    owner = e // z.nblk
    mine = e - owner * z.nblk
    last = (((1,), (1,)), ((), ()))

    def unpack(p):
        flat = jnp.dot(
            perm[...], xin[:, p].reshape(z.ep * z.xr, z.cw), preferred_element_type=F32
        ).astype(BF16)
        for q in range(z.nch):
            rows[p % 2, :, q * z.cw:(q + 1) * z.cw] = flat[q * 2 * z.rows:(q + 1) * 2 * z.rows]

    def wait_piece(p):
        landed(xin.at[pl.ds(0, z.ep - 1), p], x_recv.at[p])

    def wait_weights(p):
        if p % z.sub == 0:
            b = p // z.sub
            landed(wb.at[:, pl.ds(0, z.tp - 1), :, pl.ds(b * z.block, z.block)], w_recv.at[b])

    def project(p):
        cols = pl.ds(p * z.piece, z.piece)
        first_two = lax.dot_general(
            rows[p % 2, :z.rows], wb[:2, :, :, cols].reshape(-1, z.piece), last, preferred_element_type=F32
        )
        third = lax.dot_general(
            rows[p % 2, z.rows:], wb[2, :, :, cols].reshape(-1, z.piece), last, preferred_element_type=F32
        )
        if p:
            first_two += pout[:, :2 * z.both]
            third += pout[:, 2 * z.both:]
        pout[:, :2 * z.both] = first_two
        pout[:, 2 * z.both:] = third
        if p == z.npc - 1:
            pwire[:, :2 * z.both] = first_two.astype(BF16)
            pwire[:, 2 * z.both:] = third.astype(BF16)

    wait_piece(0)
    unpack(0)
    others = pl.ds(1, z.edp - 1)

    def spread():
        @pl.when(s == owner)
        def _():
            landed(zb, z_recv)
            for to in peers:
                send(zb.at[:, to // PARTS], rb.at[others, i], r_send, r_recv, (to, e, s))
            for k, to in enumerate(partners):
                send(zb.at[:, i // PARTS], rb.at[others, i], q_send.at[k], q_recv, (i, e, to))

    for p in range(1, z.npc):
        if p == 2:
            spread()
        if p < z.npc - 1:
            wait_piece(p)
        wait_weights(p - 1)
        if p < z.npc - 1:
            unpack(p)
        project(p - 1)
    wait_piece(z.npc - 1)
    wait_weights(z.npc - 1)
    unpack(z.npc - 1)
    project(z.npc - 1)
    for to in partners:
        send(pwire, pin.at[s], p_send, p_recv, (i, e, to))

    @pl.when(s == owner)
    def _():
        for k, to in enumerate(partners):
            send(xin.at[:, pl.ds(mine * z.sub, z.sub)], rb.at[0], q_send.at[k], q_recv, (i, e, to))


    landed(pin.at[pl.ds(0, z.tp - 1)], p_recv)
    sums = pout[...]
    for source in partners:
        sums += pin[source].astype(F32)
    gate, up, d_hidden = (sums[:, m * z.both:(m + 1) * z.both] for m in range(3))
    sig = jax.nn.sigmoid(gate)
    active = gate * sig
    hh[...] = (active * up).astype(BF16)
    hgu[:, :z.both] = (d_hidden * up * sig * (1.0 + gate * (1.0 - sig))).astype(BF16)
    hgu[:, z.both:] = (d_hidden * active).astype(BF16)

    def output(p):
        cols = pl.ds(p * z.piece, z.piece)
        out = jnp.dot(hh[...], wb[2, :, :, cols].reshape(-1, z.piece), preferred_element_type=F32)
        back = jnp.dot(hgu[...], wb[:2, :, :, cols].reshape(-1, z.piece), preferred_element_type=F32)
        for q in range(z.nch):
            for a, value in enumerate((out, back)):
                at = (2 * q + a) * z.rows
                ob[at:at + z.rows] = value[:, q * z.cw:(q + 1) * z.cw].astype(BF16)
        total = jnp.dot(perm_t[...], ob[...], preferred_element_type=F32)
        y[:, p] = total.astype(BF16).reshape(z.ep, z.xr, z.cw)
        for to in peers:
            send(y.at[to, p], yin.at[i, p], y_send, y_recv.at[p], (to, e, s))

    first = (((0,), (0,)), ((), ()))
    near = max(1, (z.edp + 1) // 2)

    def factors_out():
        for t in range(z.tp):
            at = slice(t * z.hid, (t + 1) * z.hid)
            hs[t, :z.rows] = hgu[:, at]
            hs[t, z.rows:2 * z.rows] = hgu[:, z.both + t * z.hid:z.both + (t + 1) * z.hid]
            hs[t, 2 * z.rows:] = hh[:, at]
        lb[0] = lax.dot_general(hs[s], place[...], first, preferred_element_type=F32).astype(BF16)
        upward = (2 * e) // z.edp
        for k in range(z.edp - 1):
            low = k + (k - e + z.edp) // z.edp
            high = z.edp - 1 - k
            high = high - (e - high + z.edp) // z.edp
            to = upward * low + (1 - upward) * high
            slot_at = lax.rem(e - to + z.edp, z.edp)
            send(lb.at[0], lb.at[slot_at], l_send, l_recv.at[slot_at // near], (i, to, s))

    factors_first = (2 * e) // z.edp + lax.rem(s, 2) > 0
    @pl.when(factors_first)
    def _():
        factors_out()
    output(0)
    @pl.when(~factors_first)
    def _():
        factors_out()
    for p in range(1, z.npc):
        output(p)
    yin[i] = y[i]

    @pl.when(s == owner)
    def _():
        for p in range(z.sub):
            rb[0, :, p] = xin[:, mine * z.sub + p]
        rb[1:, i] = zb[:, i // PARTS]
        landed(rb.at[others, pl.ds(0, z.ep - 1)], r_recv)
        for to in peers:
            for k, core in enumerate(partners):
                send(rb.at[others, to], rb.at[others, to], q_send.at[k], q_recv, (i, e, core))

    @pl.when(s != owner)
    def _():
        landed(rb, q_recv)

    for r in range(z.edp):
        for p in range(z.sub):
            flat = jnp.dot(
                factor[...], rb[r, :, p].reshape(z.ep * z.xr, z.cw), preferred_element_type=F32
            ).astype(BF16)
            for q in range(z.nch):
                right[pl.ds(r * z.lanes, z.lanes), pl.ds(p * z.piece + q * z.cw, z.cw)] = flat[
                    q * z.lanes:(q + 1) * z.lanes
                ]
    lane = lax.broadcasted_iota(jnp.int32, (1, z.lanes), 1)
    width = z.ep * CAP
    keeps = [((lane >= m * width) & (lane < (m + 1) * width)).astype(F32).astype(BF16) for m in range(3)]
    def weight_gradients(part):
        start = max(1, part.start)
        if part.stop > start:
            landed(lb.at[pl.ds(start, part.stop - start)], l_recv.at[part.start // near])
        factors = jnp.concatenate(
            [jnp.concatenate([lb[d] * keeps[m] for d in part], axis=1) for m in range(3)], axis=0
        )
        value = jnp.dot(
            factors, right[part.start * z.lanes:part.stop * z.lanes], preferred_element_type=F32
        )
        for m in range(3):
            rows_of = value[m * z.hid:(m + 1) * z.hid]
            wg[m] = rows_of + wg[m] if part.start else rows_of

    weight_gradients(range(near))
    for p in range(z.npc):
        landed(yin.at[pl.ds(0, z.ep - 1), p], y_recv.at[p])
        for w in range(z.window):
            total = yin[w * PARTS, p].astype(F32)
            for h in range(1, PARTS):
                total += yin[w * PARTS + h, p].astype(F32)
            summed[w, p] = (total * scales[w][1]).astype(BF16)

    weight_gradients(range(near, z.edp))

    landed(wb.at[:, pl.ds(0, z.tp - 1)], w_send)
    landed(xin.at[pl.ds(0, z.ep - 1)], x_send)
    landed(yin.at[pl.ds(0, z.ep - 1)], y_send)
    landed(pin.at[pl.ds(0, z.tp - 1)], p_send)
    landed(lb.at[others], l_send)

    @pl.when(s == owner)
    def _():
        if z.nblk > 1:
            landed(x.at[:, pl.ds(0, (z.nblk - 1) * z.sub)], z_send)
        landed(rb.at[others, pl.ds(0, z.ep - 1)], r_send)
        for k in range(z.tp - 1):
            landed(rb, q_send.at[k])

    @pl.when(s != owner)
    def _():
        landed(x, z_send)


def finish(z, wg, summed, homes, mixed, grad_tok, wgrad, mix, grad, sem):
    copies = []
    for m in range(3):
        copies.append(pltpu.make_async_copy(wg.at[m], wgrad.at[m], sem.at[m]))
        copies[-1].start()
    for p in range(z.npc):
        value = jnp.zeros((2 * z.nch * z.tok_rows, z.cw), F32)
        for w in range(z.window):
            home = homes[w].reshape(2 * z.nch * z.tok_rows, z.xr)
            value += jnp.dot(home, summed[w, p], preferred_element_type=F32)
        for q in range(z.nch):
            cols = pl.ds(p * z.piece + q * z.cw, z.cw)
            for a, target in ((0, mix), (1, grad)):
                at = (2 * q + a) * z.tok_rows
                target[:, cols] = value[at:at + z.tok_rows].astype(BF16)
    for a, target in ((0, mix), (1, grad)):
        copies.append(pltpu.make_async_copy(target, (mixed, grad_tok)[a], sem.at[3 + a]))
        copies[-1].start()
    for copy in copies:
        copy.wait()


def shards(tokens, cotangent, expert_ids, route_weights, expert_weights):
    z = Sizes(
        lax.axis_size("ep"), lax.axis_size("edp"), lax.axis_size("tp"),
        tokens.shape[0], tokens.shape[1], expert_weights.shape[1],
    )
    tables = jnp.asarray(permutations(z), BF16)
    operands = [tokens, cotangent, expert_ids.T, route_weights.T, tables, expert_weights]
    hbm = pl.BlockSpec(memory_space=pltpu.HBM)
    vmem = pl.BlockSpec(memory_space=pltpu.VMEM)
    dma = pltpu.SemaphoreType.DMA
    passed = pl.pallas_call(
        functools.partial(kernel, z),
        out_shape=(
            pltpu.VMEM((3, z.hid, z.block), F32),
            pltpu.VMEM((z.window, z.npc, z.xr, z.cw), BF16),
            pltpu.VMEM((z.window, 2 * z.nch, z.tok_rows, z.xr), BF16),
        ),
        in_specs=[hbm] * len(operands),
        out_specs=(vmem,) * 3,
        scratch_shapes=[
            pltpu.VMEM((2, *tokens.shape), BF16),
            *(pltpu.VMEM(o.shape, o.dtype) for o in operands[2:5]),
            pltpu.VMEM((3, z.tp, z.hid, z.feats), BF16),
            pltpu.VMEM((z.window, z.npc, z.xr, z.cw), BF16),
            pltpu.VMEM((z.ep, z.npc, z.xr, z.cw), BF16),
            pltpu.VMEM((z.edp - 1, z.window, z.sub, z.xr, z.cw), BF16),
            pltpu.VMEM((z.edp, z.ep, z.sub, z.xr, z.cw), BF16),
            pltpu.VMEM((2, 2 * z.rows, z.piece), BF16),
            pltpu.VMEM((z.rows, 3 * z.both), F32),
            pltpu.VMEM((z.rows, 3 * z.both), BF16),
            pltpu.VMEM((z.tp, z.rows, 3 * z.both), BF16),
            pltpu.VMEM((z.rows, 2 * z.both), BF16),
            pltpu.VMEM((z.rows, z.both), BF16),
            pltpu.VMEM((z.tp, 3 * z.rows, z.hid), BF16),
            pltpu.VMEM((z.edp, z.hid, z.lanes), BF16),
            pltpu.VMEM((z.nch * 2 * z.rows, z.cw), BF16),
            pltpu.VMEM((z.ep, z.npc, z.xr, z.cw), BF16),
            pltpu.VMEM((z.ep, z.npc, z.xr, z.cw), BF16),
            pltpu.VMEM((z.edp * z.lanes, z.block), BF16),
            dma((5,)), dma, dma, dma((z.nblk,)), dma, dma((z.npc,)), dma, dma, dma, dma, dma, dma,
            dma, dma((2,)), dma, dma((z.npc,)), dma((z.tp - 1,)), dma,
            pltpu.SemaphoreType.REGULAR, pltpu.SemaphoreType.REGULAR, pltpu.SemaphoreType.REGULAR,
        ],
        compiler_params=pltpu.CompilerParams(
            collective_id=0, has_side_effects=True, vmem_limit_bytes=VMEM_LIMIT
        ),
        name="expert_block",
    )(*[pltpu.with_memory_space_constraint(o, pltpu.HBM) for o in operands])
    return pl.pallas_call(
        functools.partial(finish, z),
        out_shape=(
            jax.ShapeDtypeStruct(tokens.shape, BF16),
            jax.ShapeDtypeStruct(tokens.shape, BF16),
            jax.ShapeDtypeStruct((3, z.hid, z.block), F32),
        ),
        in_specs=[vmem] * 3,
        out_specs=(hbm,) * 3,
        scratch_shapes=[
            pltpu.VMEM(tokens.shape, BF16),
            pltpu.VMEM(tokens.shape, BF16),
            dma((5,)),
        ],
        compiler_params=pltpu.CompilerParams(vmem_limit_bytes=VMEM_LIMIT),
        name="finish",
    )(*[pltpu.with_memory_space_constraint(o, pltpu.VMEM) for o in passed])


def solution(mesh):
    placed = (
        P(("ep", "edp"), "tp"),
        P(("ep", "edp"), "tp"),
        P(("ep", "edp"), None),
        P(("ep", "edp"), None),
        P(None, ("ep", "tp"), None),
    )
    return jax.shard_map(
        shards,
        mesh=mesh,
        in_specs=placed,
        out_specs=(P(("ep", "edp"), "tp"), P(("ep", "edp"), "tp"), P(None, ("ep", "tp"), "edp")),
        check_vma=False,
    )
```

```python
import functools
import math

import jax
import jax.numpy as jnp
import numpy as np
from jax import lax
from jax.experimental import pallas as pl
from jax.experimental.pallas import tpu as pltpu
from jax.sharding import PartitionSpec as P

CAP = 10
PARTS = 4
SUB = 2
VMEM_LIMIT = 40 * 1024 * 1024
MESH = pl.DeviceIdType.MESH
F32 = jnp.float32
BF16 = jnp.bfloat16


def round_up(value, unit):
    return -(-value // unit) * unit


class Sizes:
    def __init__(self, ep, edp, tp, tok_rows, feats, hid):
        self.ep, self.edp, self.tp = ep, edp, tp
        self.window = ep // PARTS
        self.tok_rows, self.feats, self.hid = tok_rows, feats, hid
        self.block = feats * tp // edp
        self.nblk = feats // self.block
        self.sub = SUB if self.block % (SUB * 512) == 0 else 1
        self.piece = self.block // self.sub
        self.npc = feats // self.piece
        self.nch = max(1, min(4, self.piece // 128, max(2, self.piece // 256)))
        self.cw = self.piece // self.nch
        self.xr = round_up(2 * CAP * self.nch, 8)
        self.rows = round_up(ep * CAP, 16)
        self.lanes = round_up(3 * ep * CAP, 128)
        self.both = tp * hid
        wide, tall = ep * self.xr, self.nch * 2 * self.rows
        self.tables, at = [], 0
        for n, width in ((tall, wide), (wide, tall), (self.nch * self.lanes, wide), (3 * self.rows, self.lanes)):
            self.tables.append((at, n, width))
            at += n
        self.table_lanes = round_up(max(width for _, _, width in self.tables), 128)
        side = math.isqrt(ep)
        side = side if side * side == ep else ep
        steps = [(a, b) for a in range(ep // side) for b in range(side) if a or b]
        self.side, self.steps = side, sorted(steps, key=lambda ab: -(bool(ab[0]) + bool(ab[1])))


def permutations(z):
    table = np.zeros((z.nch, 2, z.rows, z.ep, z.xr), np.float32)
    factor = np.zeros((z.nch, z.lanes, z.ep, z.xr), np.float32)
    place = np.zeros((3, z.rows, z.lanes), np.float32)
    for i in range(z.ep):
        for c in range(CAP):
            for q in range(z.nch):
                for a in range(2):
                    table[q, a, i * CAP + c, i, (2 * q + a) * CAP + c] = 1.0
                for m in range(3):
                    factor[q, (m * z.ep + i) * CAP + c, i, (2 * q + m // 2) * CAP + c] = 1.0
            for m in range(3):
                place[m, i * CAP + c, (m * z.ep + i) * CAP + c] = 1.0
    flat = table.reshape(z.nch * 2 * z.rows, z.ep * z.xr)
    packed = np.zeros((sum(n for _, n, _ in z.tables), z.table_lanes), np.float32)
    for (at, n, width), part in zip(z.tables, (flat, flat.T, factor, place), strict=True):
        packed[at:at + n, :width] = part.reshape(n, width)
    return packed


def slot_parts(index, nch):
    chunk = jnp.zeros_like(index)
    for k in range(1, nch):
        chunk += (index >= 2 * CAP * k).astype(jnp.int32)
    rest = index - 2 * CAP * chunk
    array = (rest >= CAP).astype(jnp.int32)
    return chunk, array, rest - CAP * array


def landed(ref, sem):
    pltpu.make_async_copy(ref, ref, sem).wait()


def kernel(
    z, tok_in, cot_in, ids_in, rw_in, tables_in, weights,
    wg, summed, homes,
    data, ids, rw, tables,
    wb, x, xin, zb, rb, rows, pout, pwire, pin, hgu, hh, hs, lb, ob, y, yin, right,
    in_sem, w_loc, w_send, w_recv, x_send, x_recv, z_send, z_recv, r_send, r_recv, p_send, p_recv,
    l_send, l_recv, y_send, y_recv, q_send, q_recv, core_ready, plane_ready, edp_ready, turn,
):
    i, e, s = lax.axis_index("ep"), lax.axis_index("edp"), lax.axis_index("tp")
    barrier = pltpu.get_barrier_semaphore()
    down, across = i // z.side, lax.rem(i, z.side)
    peers = [
        lax.rem(down + a, z.ep // z.side) * z.side + lax.rem(across + b, z.side) for a, b in z.steps
    ]
    partners = [lax.rem(s + d, z.tp) for d in range(1, z.tp)]
    perm, perm_t, factor, place = (tables.at[pl.ds(at, n), pl.ds(0, width)] for at, n, width in z.tables)

    loads = [
        pltpu.make_async_copy(ids_in, ids, in_sem.at[0]),
        pltpu.make_async_copy(rw_in, rw, in_sem.at[1]),
    ]
    head, rest = pl.ds(0, z.piece), pl.ds(z.piece, z.feats - z.piece)
    for k, cols in enumerate((head, rest)):
        loads.append(pltpu.make_async_copy(tok_in.at[:, cols], data.at[0, :, cols], in_sem.at[2 + k]))
        loads.append(pltpu.make_async_copy(cot_in.at[:, cols], data.at[1, :, cols], in_sem.at[2 + k]))
    for copy in loads:
        copy.start()

    def signal(semaphore, to):
        pl.semaphore_signal(semaphore, inc=1, device_id=to, device_id_type=MESH)

    last_core = z.tp - 1
    lead = s == last_core
    @pl.when(lead)
    def _():
        for t in range(last_core):
            signal(barrier, (i, e, t))

    for to in peers:
        signal(barrier, (to, e, last_core))
    for d in range(1, z.edp):
        @pl.when(e + d < z.edp)
        def _():
            signal(barrier, (i, lax.rem(e + d, z.edp), 0))

    @pl.when(s == 0)
    def _():
        pl.semaphore_wait(barrier, 1 + e * z.tp)

    @pl.when((s != 0) & (s != last_core))
    def _():
        pl.semaphore_wait(barrier, 1)

    @pl.when(s != last_core)
    def _():
        signal(core_ready, (i, e, last_core))
        if z.tp > 2:
            pl.semaphore_wait(core_ready, 1)

    @pl.when(lead)
    def _():
        pl.semaphore_wait(core_ready, last_core)
        if z.tp > 2:
            for t in range(last_core):
                signal(core_ready, (i, e, t))

    @pl.when(s == 0)
    def _():
        for d in range(1, z.edp):
            @pl.when(e - d >= 0)
            def _():
                for t in range(z.tp):
                    signal(edp_ready, (i, lax.rem(e - d + z.edp, z.edp), t))

    def enter():
        @pl.when(lead)
        def _():
            pl.semaphore_wait(barrier, (z.ep - 1) * z.tp)
            for t in range(last_core):
                signal(plane_ready, (i, e, t))

        @pl.when(s != last_core)
        def _():
            pl.semaphore_wait(plane_ready, 1)

    def send(source, target, send_sem, recv_sem, to):
        pltpu.make_async_remote_copy(
            src_ref=source, dst_ref=target, send_sem=send_sem, recv_sem=recv_sem,
            device_id=to, device_id_type=MESH,
        ).start()

    for b in range(z.nblk):
        for to in partners:
            cols = pl.ds(pl.multiple_of(to * z.feats + b * z.block, 128), z.block)
            send(
                weights.at[:, :, cols], wb.at[:, s, :, pl.ds(b * z.block, z.block)],
                w_send, w_recv.at[b], (i, e, to),
            )

    row = lax.broadcasted_iota(jnp.int32, (z.xr, z.tok_rows), 0)
    chunk, array, slot = slot_parts(row, z.nch)
    in_use = row < 2 * CAP * z.nch
    before = (
        lax.broadcasted_iota(jnp.int32, (z.tok_rows, z.tok_rows), 0)
        < lax.broadcasted_iota(jnp.int32, (z.tok_rows, z.tok_rows), 1)
    ).astype(F32).astype(BF16)
    lane = lax.broadcasted_iota(jnp.int32, (z.tok_rows, z.xr), 1)
    lane_chunk, lane_array, _ = slot_parts(lane, z.nch)
    loads[0].wait()
    loads[1].wait()
    ids_t = ids[...]
    rw_t = rw[...]
    chosen, scales, picks = [], [], []
    for w in range(z.window):
        hit = (ids_t == w).astype(F32)
        match = jnp.sum(hit, axis=0, keepdims=True)
        weight = jnp.sum(hit * rw_t, axis=0, keepdims=True)
        match_all = jnp.broadcast_to(match, (z.xr, z.tok_rows))
        rank = jnp.dot(match_all.astype(BF16), before, preferred_element_type=F32)
        pick = jnp.where(in_use & (rank == slot.astype(F32)), match_all, 0.0)
        slot_weight = jnp.sum(pick * weight, axis=1, keepdims=True)
        picks.append(pick)
        scales.append((
            jnp.where(array[:, :1] == 1, slot_weight, 1.0), jnp.where(array[:, :1] == 0, slot_weight, 1.0),
        ))
        chosen.append([
            [jnp.where((chunk == q) & (array == a), pick, 0.0).astype(BF16) for a in range(2)]
            for q in range(z.nch)
        ])
    landed(data.at[:, :, head], in_sem.at[2])
    own_w = pltpu.make_async_copy(
        weights.at[:, :, pl.ds(pl.multiple_of(s * z.feats, 128), z.feats)], wb.at[:, s], w_loc
    )
    table_load = pltpu.make_async_copy(tables_in, tables, in_sem.at[4])

    def send_rows(p, to):
        send(x.at[to // PARTS, p], xin.at[i, p], x_send.at[min(p, 1)], x_recv.at[p], (to, e, s))

    def send_replica(b):
        to = s * z.nblk + b
        slot_at = lax.rem(e - to + z.edp, z.edp) - 1
        send(x.at[:, pl.ds(b * z.sub, z.sub)], zb.at[slot_at], z_send, z_recv, (i, to, s))

    for p in range(z.npc):
        if p == 1:
            landed(data.at[:, :, rest], in_sem.at[3])
            own_w.start()
            table_load.start()
        for w in range(z.window):
            total = jnp.zeros((z.xr, z.cw), F32)
            for q in range(z.nch):
                cols = pl.ds(p * z.piece + q * z.cw, z.cw)
                for a in range(2):
                    total += jnp.dot(chosen[w][q][a], data[a, :, cols], preferred_element_type=F32)
            x[w, p] = (total * scales[w][0]).astype(BF16)
        if p % z.sub == z.sub - 1:
            @pl.when(s * z.nblk + p // z.sub < e)
            def _():
                send_replica(p // z.sub)

    enter()

    ahead = max(1, z.npc - 1)

    def send_pieces(pieces):
        for p in pieces:
            for to in peers:
                send_rows(p, to)

    def first_piece_left():
        landed(xin.at[pl.ds(0, z.ep - 1), 0], x_send.at[0])

    second = lax.rem(s, 2) == 1
    has_second = (~second) & (s + 1 < z.tp)
    send_pieces(range(1))

    @pl.when(~second)
    def _():
        send_pieces(range(1, z.npc))

    @pl.when(second)
    def _():
        send_pieces(range(1, ahead))

    for p in range(z.npc):
        xin[i, p] = x[i // PARTS, p]
    for w in range(z.window):
        home = jnp.transpose(picks[w])
        for q in range(z.nch):
            for a in range(2):
                homes[w, 2 * q + a] = jnp.where(
                    (lane_chunk == q) & (lane_array == a), home, 0.0
                ).astype(BF16)

    @pl.when(has_second)
    def _():
        first_piece_left()
        signal(turn, (i, e, s + 1))

    @pl.when(second)
    def _():
        pl.semaphore_wait(turn, 1)
        send_pieces(range(ahead, z.npc))

    @pl.when(e < z.edp - 1)
    def _():
        pl.semaphore_wait(edp_ready, z.edp - 1 - e)

    for b in range(z.nblk):
        @pl.when(s * z.nblk + b > e)
        def _():
            send_replica(b)
    own_w.wait()
    table_load.wait()

    owner = e // z.nblk
    mine = e - owner * z.nblk
    last = (((1,), (1,)), ((), ()))

    def unpack(p):
        flat = jnp.dot(
            perm[...], xin[:, p].reshape(z.ep * z.xr, z.cw), preferred_element_type=F32
        ).astype(BF16)
        for q in range(z.nch):
            rows[p % 2, :, q * z.cw:(q + 1) * z.cw] = flat[q * 2 * z.rows:(q + 1) * 2 * z.rows]

    def wait_piece(p):
        landed(xin.at[pl.ds(0, z.ep - 1), p], x_recv.at[p])

    def wait_weights(p):
        if p % z.sub == 0:
            b = p // z.sub
            landed(wb.at[:, pl.ds(0, z.tp - 1), :, pl.ds(b * z.block, z.block)], w_recv.at[b])

    def project(p):
        cols = pl.ds(p * z.piece, z.piece)
        first_two = lax.dot_general(
            rows[p % 2, :z.rows], wb[:2, :, :, cols].reshape(-1, z.piece), last, preferred_element_type=F32
        )
        third = lax.dot_general(
            rows[p % 2, z.rows:], wb[2, :, :, cols].reshape(-1, z.piece), last, preferred_element_type=F32
        )
        if p:
            first_two += pout[:, :2 * z.both]
            third += pout[:, 2 * z.both:]
        pout[:, :2 * z.both] = first_two
        pout[:, 2 * z.both:] = third
        if p == z.npc - 1:
            pwire[:, :2 * z.both] = first_two.astype(BF16)
            pwire[:, 2 * z.both:] = third.astype(BF16)

    wait_piece(0)
    unpack(0)
    others = pl.ds(1, z.edp - 1)

    def spread():
        @pl.when(s == owner)
        def _():
            landed(zb, z_recv)
            for to in peers:
                send(zb.at[:, to // PARTS], rb.at[others, i], r_send, r_recv, (to, e, s))
            for k, to in enumerate(partners):
                send(zb.at[:, i // PARTS], rb.at[others, i], q_send.at[k], q_recv, (i, e, to))

    for p in range(1, z.npc):
        if p == 2:
            spread()
        if p < z.npc - 1:
            wait_piece(p)
        wait_weights(p - 1)
        if p < z.npc - 1:
            unpack(p)
        project(p - 1)
    wait_piece(z.npc - 1)
    wait_weights(z.npc - 1)
    unpack(z.npc - 1)
    project(z.npc - 1)
    for to in partners:
        send(pwire, pin.at[s], p_send, p_recv, (i, e, to))

    @pl.when(s == owner)
    def _():
        for k, to in enumerate(partners):
            send(xin.at[:, pl.ds(mine * z.sub, z.sub)], rb.at[0], q_send.at[k], q_recv, (i, e, to))


    landed(pin.at[pl.ds(0, z.tp - 1)], p_recv)
    sums = pout[...]
    for source in partners:
        sums += pin[source].astype(F32)
    gate, up, d_hidden = (sums[:, m * z.both:(m + 1) * z.both] for m in range(3))
    sig = jax.nn.sigmoid(gate)
    active = gate * sig
    hh[...] = (active * up).astype(BF16)
    hgu[:, :z.both] = (d_hidden * up * sig * (1.0 + gate * (1.0 - sig))).astype(BF16)
    hgu[:, z.both:] = (d_hidden * active).astype(BF16)

    def output(p):
        cols = pl.ds(p * z.piece, z.piece)
        out = jnp.dot(hh[...], wb[2, :, :, cols].reshape(-1, z.piece), preferred_element_type=F32)
        back = jnp.dot(hgu[...], wb[:2, :, :, cols].reshape(-1, z.piece), preferred_element_type=F32)
        for q in range(z.nch):
            for a, value in enumerate((out, back)):
                at = (2 * q + a) * z.rows
                ob[at:at + z.rows] = value[:, q * z.cw:(q + 1) * z.cw].astype(BF16)
        total = jnp.dot(perm_t[...], ob[...], preferred_element_type=F32)
        y[:, p] = total.astype(BF16).reshape(z.ep, z.xr, z.cw)
        for to in peers:
            send(y.at[to, p], yin.at[i, p], y_send, y_recv.at[p], (to, e, s))

    first = (((0,), (0,)), ((), ()))
    def factors_out():
        for t in range(z.tp):
            at = slice(t * z.hid, (t + 1) * z.hid)
            hs[t, :z.rows] = hgu[:, at]
            hs[t, z.rows:2 * z.rows] = hgu[:, z.both + t * z.hid:z.both + (t + 1) * z.hid]
            hs[t, 2 * z.rows:] = hh[:, at]
        lb[0] = lax.dot_general(hs[s], place[...], first, preferred_element_type=F32).astype(BF16)
        upward = (2 * e) // z.edp
        for k in range(z.edp - 1):
            low = k + (k - e + z.edp) // z.edp
            high = z.edp - 1 - k
            high = high - (e - high + z.edp) // z.edp
            to = upward * low + (1 - upward) * high
            slot_at = lax.rem(e - to + z.edp, z.edp)
            send(lb.at[0], lb.at[slot_at], l_send, l_recv.at[slot_at], (i, to, s))

    factors_first = (2 * e) // z.edp + lax.rem(s, 2) > 0
    @pl.when(factors_first)
    def _():
        factors_out()
    output(0)
    @pl.when(~factors_first)
    def _():
        factors_out()
    for p in range(1, z.npc):
        output(p)
    yin[i] = y[i]

    @pl.when(s == owner)
    def _():
        for p in range(z.sub):
            rb[0, :, p] = xin[:, mine * z.sub + p]
        rb[1:, i] = zb[:, i // PARTS]
        landed(rb.at[others, pl.ds(0, z.ep - 1)], r_recv)
        for to in peers:
            for k, core in enumerate(partners):
                send(rb.at[others, to], rb.at[others, to], q_send.at[k], q_recv, (i, e, core))

    @pl.when(s != owner)
    def _():
        landed(rb, q_recv)

    for r in range(z.edp):
        for p in range(z.sub):
            flat = jnp.dot(
                factor[...], rb[r, :, p].reshape(z.ep * z.xr, z.cw), preferred_element_type=F32
            ).astype(BF16)
            for q in range(z.nch):
                right[pl.ds(r * z.lanes, z.lanes), pl.ds(p * z.piece + q * z.cw, z.cw)] = flat[
                    q * z.lanes:(q + 1) * z.lanes
                ]
    lane = lax.broadcasted_iota(jnp.int32, (1, z.lanes), 1)
    width = z.ep * CAP
    keeps = [((lane >= m * width) & (lane < (m + 1) * width)).astype(F32).astype(BF16) for m in range(3)]
    near = max(1, z.edp // 2)
    for part in (range(near), range(near, z.edp)):
        for d in part:
            if d:
                landed(lb.at[d], l_recv.at[d])
        for m in range(3):
            factors = jnp.concatenate([lb[d] * keeps[m] for d in part], axis=1)
            value = jnp.dot(
                factors, right[part.start * z.lanes:part.stop * z.lanes], preferred_element_type=F32
            )
            if part.start:
                value += wg[m]
            wg[m] = value

    for p in range(z.npc):
        landed(yin.at[pl.ds(0, z.ep - 1), p], y_recv.at[p])
        for w in range(z.window):
            total = yin[w * PARTS, p].astype(F32)
            for h in range(1, PARTS):
                total += yin[w * PARTS + h, p].astype(F32)
            summed[w, p] = (total * scales[w][1]).astype(BF16)

    landed(wb.at[:, pl.ds(0, z.tp - 1)], w_send)
    landed(xin.at[pl.ds(0, z.ep - 1), pl.ds(1, z.npc - 1)], x_send.at[1])

    @pl.when(~has_second)
    def _():
        first_piece_left()

    landed(yin.at[pl.ds(0, z.ep - 1)], y_send)
    landed(pin.at[pl.ds(0, z.tp - 1)], p_send)
    landed(lb.at[others], l_send)

    @pl.when(s == owner)
    def _():
        if z.nblk > 1:
            landed(x.at[:, pl.ds(0, (z.nblk - 1) * z.sub)], z_send)
        landed(rb.at[others, pl.ds(0, z.ep - 1)], r_send)
        for k in range(z.tp - 1):
            landed(rb, q_send.at[k])

    @pl.when(s != owner)
    def _():
        landed(x, z_send)


def finish(z, wg, summed, homes, mixed, grad_tok, wgrad, mix, grad, sem):
    copies = []
    for m in range(3):
        copies.append(pltpu.make_async_copy(wg.at[m], wgrad.at[m], sem.at[m]))
        copies[-1].start()
    for p in range(z.npc):
        value = jnp.zeros((2 * z.nch * z.tok_rows, z.cw), F32)
        for w in range(z.window):
            home = homes[w].reshape(2 * z.nch * z.tok_rows, z.xr)
            value += jnp.dot(home, summed[w, p], preferred_element_type=F32)
        for q in range(z.nch):
            cols = pl.ds(p * z.piece + q * z.cw, z.cw)
            for a, target in ((0, mix), (1, grad)):
                at = (2 * q + a) * z.tok_rows
                target[:, cols] = value[at:at + z.tok_rows].astype(BF16)
    for a, target in ((0, mix), (1, grad)):
        copies.append(pltpu.make_async_copy(target, (mixed, grad_tok)[a], sem.at[3 + a]))
        copies[-1].start()
    for copy in copies:
        copy.wait()


def shards(tokens, cotangent, expert_ids, route_weights, expert_weights):
    z = Sizes(
        lax.axis_size("ep"), lax.axis_size("edp"), lax.axis_size("tp"),
        tokens.shape[0], tokens.shape[1], expert_weights.shape[1],
    )
    tables = jnp.asarray(permutations(z), BF16)
    operands = [tokens, cotangent, expert_ids.T, route_weights.T, tables, expert_weights]
    hbm = pl.BlockSpec(memory_space=pltpu.HBM)
    vmem = pl.BlockSpec(memory_space=pltpu.VMEM)
    dma = pltpu.SemaphoreType.DMA
    passed = pl.pallas_call(
        functools.partial(kernel, z),
        out_shape=(
            pltpu.VMEM((3, z.hid, z.block), F32),
            pltpu.VMEM((z.window, z.npc, z.xr, z.cw), BF16),
            pltpu.VMEM((z.window, 2 * z.nch, z.tok_rows, z.xr), BF16),
        ),
        in_specs=[hbm] * len(operands),
        out_specs=(vmem,) * 3,
        scratch_shapes=[
            pltpu.VMEM((2, *tokens.shape), BF16),
            *(pltpu.VMEM(o.shape, o.dtype) for o in operands[2:5]),
            pltpu.VMEM((3, z.tp, z.hid, z.feats), BF16),
            pltpu.VMEM((z.window, z.npc, z.xr, z.cw), BF16),
            pltpu.VMEM((z.ep, z.npc, z.xr, z.cw), BF16),
            pltpu.VMEM((z.edp - 1, z.window, z.sub, z.xr, z.cw), BF16),
            pltpu.VMEM((z.edp, z.ep, z.sub, z.xr, z.cw), BF16),
            pltpu.VMEM((2, 2 * z.rows, z.piece), BF16),
            pltpu.VMEM((z.rows, 3 * z.both), F32),
            pltpu.VMEM((z.rows, 3 * z.both), BF16),
            pltpu.VMEM((z.tp, z.rows, 3 * z.both), BF16),
            pltpu.VMEM((z.rows, 2 * z.both), BF16),
            pltpu.VMEM((z.rows, z.both), BF16),
            pltpu.VMEM((z.tp, 3 * z.rows, z.hid), BF16),
            pltpu.VMEM((z.edp, z.hid, z.lanes), BF16),
            pltpu.VMEM((z.nch * 2 * z.rows, z.cw), BF16),
            pltpu.VMEM((z.ep, z.npc, z.xr, z.cw), BF16),
            pltpu.VMEM((z.ep, z.npc, z.xr, z.cw), BF16),
            pltpu.VMEM((z.edp * z.lanes, z.block), BF16),
            dma((5,)), dma, dma, dma((z.nblk,)), dma((2,)), dma((z.npc,)), dma, dma, dma, dma, dma, dma,
            dma, dma((z.edp,)), dma, dma((z.npc,)), dma((z.tp - 1,)), dma,
            *[pltpu.SemaphoreType.REGULAR] * 4,
        ],
        compiler_params=pltpu.CompilerParams(
            collective_id=0, has_side_effects=True, vmem_limit_bytes=VMEM_LIMIT
        ),
        name="expert_block",
    )(*[pltpu.with_memory_space_constraint(o, pltpu.HBM) for o in operands])
    return pl.pallas_call(
        functools.partial(finish, z),
        out_shape=(
            jax.ShapeDtypeStruct(tokens.shape, BF16),
            jax.ShapeDtypeStruct(tokens.shape, BF16),
            jax.ShapeDtypeStruct((3, z.hid, z.block), F32),
        ),
        in_specs=[vmem] * 3,
        out_specs=(hbm,) * 3,
        scratch_shapes=[
            pltpu.VMEM(tokens.shape, BF16),
            pltpu.VMEM(tokens.shape, BF16),
            dma((5,)),
        ],
        compiler_params=pltpu.CompilerParams(vmem_limit_bytes=VMEM_LIMIT),
        name="finish",
    )(*[pltpu.with_memory_space_constraint(o, pltpu.VMEM) for o in passed])


def solution(mesh):
    placed = (
        P(("ep", "edp"), "tp"),
        P(("ep", "edp"), "tp"),
        P(("ep", "edp"), None),
        P(("ep", "edp"), None),
        P(None, ("ep", "tp"), None),
    )
    return jax.shard_map(
        shards,
        mesh=mesh,
        in_specs=placed,
        out_specs=(P(("ep", "edp"), "tp"), P(("ep", "edp"), "tp"), P(None, ("ep", "tp"), "edp")),
        check_vma=False,
    )
```
